256 devices in a mesh: col: 4 (over y), tile: 64 (over x, z, core).
Axes of the slice: x: 4, y: 4, z: 8, core: 2. Of those that a mesh axis runs over, the one named last changes fastest.
Arguments:
- vectors: float32 [8, 4, 512, 2048], P(None, None, 'tile', 'col'), may hold values from -12 to 12
- onsite: float32 [4, 512, 2048], P(None, 'tile', 'col'), may hold values from -0.3 to 0.3
- intra_hop: float32 [3, 2, 512, 2048], P(None, None, 'tile', 'col'), may hold values from 0.15 to 0.35
- inter_index: int32 [4, 2, 512, 2048], P(None, None, 'tile', 'col'), may hold values from 0 to 18
- inter_hop: float32 [4, 2, 512, 2048], P(None, None, 'tile', 'col'), may hold values from 0.04 to 0.16
Outputs:
- last_term: float32 [8, 4, 512, 2048], P(None, None, 'tile', 'col')
- moments: float32 [7, 8], replicated
The draws below stay inside these ranges and needn't reach their ends.
Inputs may be any that keep to these rules, and one draw needn't show every extreme that they name: `inter_index`: A code c below 18 names the second-layer orbital of sublattice c // 9 in the cell at offset ((c % 9) // 3 - 1, c % 3 - 1) from the slot's cell; 18 marks an empty slot.
All inputs are finite; a program needn't handle non-finite values.
Results may differ from the reference program's by a relative error of at most 0.000025.
Values sent between devices are 32-bit elements; how exact they have to be, the bound alone decides.
No kernel may reach another device: no remote copies, remote signals or barrier semaphores. Data moves between devices by JAX's collectives and lax.ppermute only.
A program may use at most 64 MiB of HBM per device.

```python
import jax
import jax.numpy as jnp

VECS = 8
K = 4
NA = 512
NB = 2048


def draw_vectors(key, part):
    first_key = jax.random.fold_in(jax.random.fold_in(key, 7), 0)
    positions = jnp.arange(NA, dtype=jnp.float32) / NA
    ramp = jnp.exp(jnp.log(3.0) * positions)[:, None]
    base = jnp.clip(jax.random.normal(first_key, (VECS, 4, NA, NB), jnp.float32), -4.0, 4.0)
    return base * ramp


def touch_ends(values, key, low, largest):
    index_at = [jax.random.randint(jax.random.fold_in(key, axis), (), 0, length) for axis, length in enumerate(values.shape)]
    longest = values.shape.index(max(values.shape))
    neighbour = index_at[:longest] + [(index_at[longest] + 1) % values.shape[longest]] + index_at[longest + 1:]
    return values.at[tuple(index_at)].set(low).at[tuple(neighbour)].set(largest)


def shard_levels(own_key, extent, cuts, least, high):
    def one(axis_at, shards_of):
        draws = jax.random.uniform(jax.random.fold_in(jax.random.fold_in(own_key, 6), axis_at), (shards_of,), jnp.float32, least / len(cuts), high / len(cuts))
        return jnp.repeat(jnp.exp(draws), extent[axis_at] // shards_of).reshape((-1,) + (1,) * (len(extent) - axis_at - 1))

    level = one(*cuts[0])
    for cut in cuts[1:]:
        level = level * one(*cut)
    return level


def setup_inputs(seed: int = 0) -> dict:
    seeds = jax.random.split(jax.random.key(seed), 6)
    vectors = draw_vectors(jax.random.fold_in(seeds[5], 71), 0)
    onsite = jnp.clip(jax.random.uniform(seeds[1], (4, NA, NB), jnp.float32, -0.3, 0.3) * shard_levels(seeds[1], (4, NA, NB), ((1, 64), (2, 4)), -0.4, 0.0), -0.3, 0.3)
    intra_hop = jnp.clip(0.15 + 0.19999999 * jax.random.uniform(seeds[2], (3, 2, NA, NB), jnp.float32) ** shard_levels(seeds[2], (3, 2, NA, NB), ((2, 64), (3, 4)), -0.2, 0.2), 0.15, 0.35)
    inter_index = touch_ends(jax.random.randint(seeds[3], (K, 2, NA, NB), 0, 19), jax.random.fold_in(seeds[3], 1), 0, 18).astype(jnp.int32)
    inter_hop = jnp.clip(0.04 + 0.12 * jax.random.uniform(seeds[4], (K, 2, NA, NB), jnp.float32) ** shard_levels(seeds[4], (K, 2, NA, NB), ((2, 64), (3, 4)), -0.2, 0.2), 0.04, 0.16)
    return {"vectors": vectors, "onsite": onsite, "intra_hop": intra_hop, "inter_index": inter_index, "inter_hop": inter_hop}


BOND_OFFSETS = ((0, 0), (-1, 0), (0, -1))


def rolled(array, row_off, col_off):
    return jnp.roll(array, (-row_off, -col_off), axis=(-2, -1))


def make_weights(neighbours, amplitude):
    return jnp.stack([jnp.sum(jnp.where(neighbours == code_no, amplitude, jnp.zeros_like(amplitude)), axis=0) for code_no in range(18)], axis=1)


def apply_hamiltonian(vector, onsite, intra_hop, weights, pick):
    outputs = []
    for layer_no in range(2):
        side_a = vector[:, 2 * layer_no]
        side_b = vector[:, 2 * layer_no + 1]
        out_a = pick(onsite[2 * layer_no], 0, 0) * pick(side_a, 0, 0)
        out_b = pick(onsite[2 * layer_no + 1], 0, 0) * pick(side_b, 0, 0)
        for bond_idx in range(3):
            row_off, col_off = BOND_OFFSETS[bond_idx]
            out_a = out_a + pick(intra_hop[bond_idx, layer_no], 0, 0) * pick(side_b, row_off, col_off)
            out_b = out_b + pick(intra_hop[bond_idx, layer_no], -row_off, -col_off) * pick(side_a, -row_off, -col_off)
        outputs += [out_a, out_b]
    for source in range(2):
        for code_no in range(18):
            target = code_no // 9
            row_off = (code_no % 9) // 3 - 1
            col_off = code_no % 3 - 1
            outputs[source] = outputs[source] + pick(weights[source, code_no], 0, 0) * pick(vector[:, 2 + target], row_off, col_off)
            outputs[2 + target] = outputs[2 + target] + pick(weights[source, code_no], -row_off, -col_off) * pick(vector[:, source], -row_off, -col_off)
    return jnp.stack(outputs, axis=1)


def inner_sums(left, right):
    return jnp.sum(left * right, axis=(1, 2, 3))


def moments_from(totals, orbitals):
    scaled = totals / orbitals
    zeroth = scaled[0]
    first = scaled[1]
    return jnp.stack([zeroth, first, 2.0 * scaled[2] - zeroth, 2.0 * scaled[3] - first, 2.0 * scaled[4] - zeroth, 2.0 * scaled[5] - first, 2.0 * scaled[6] - zeroth])


def reference(vectors, onsite, intra_hop, inter_index, inter_hop):
    weights = make_weights(inter_index, inter_hop)

    def operator(vector):
        return apply_hamiltonian(vector, onsite, intra_hop, weights, rolled)

    term_zero = vectors
    term_one = operator(term_zero)
    term_two = 2.0 * operator(term_one) - term_zero
    last_term = 2.0 * operator(term_two) - term_one
    totals = jnp.stack([inner_sums(term_zero, term_zero), inner_sums(term_one, term_zero), inner_sums(term_one, term_one), inner_sums(term_two, term_one), inner_sums(term_two, term_two), inner_sums(last_term, term_two), inner_sums(last_term, last_term)])
    return last_term, moments_from(totals, 4 * NA * NB)
```

```python
import functools

import jax
import jax.numpy as jnp
from jax import lax
from jax.experimental import pallas as pl
from jax.experimental.pallas import tpu as pltpu
from jax.sharding import Mesh
from jax.sharding import PartitionSpec as P

TILE = ("tile_0", "tile_1", "tile_2")
EVERY = ("col",) + TILE

V = 8
R = 8
C = 512
W = C + 128
RING = 16
RIM = 3
COEFS = 26
LANES = 128
FIELD_ROWS = 4 * RIM * V
ROW_MSG = FIELD_ROWS + COEFS * 4

FWD = 0
SHIFTED = 36
INTRA = 60
INTRA_SHIFTED = 66
ONSITE = 68
PLANES = 72

SIDE_CODES = [code for code in range(18) if code % 3 != 1]


def offsets(code):
    return code % 9 // 3 - 1, code % 3 - 1


def shifted_plane(source, code):
    if code % 3 == 1:
        return FWD + source * 18 + code
    return SHIFTED + source * 12 + SIDE_CODES.index(code)


def lanes_of(shape):
    return lax.broadcasted_iota(jnp.int32, shape, len(shape) - 1)


def subs_of(shape):
    return lax.broadcasted_iota(jnp.int32, shape, len(shape) - 2)


def lane_roll(array, amount):
    amount = amount % array.shape[-1]
    if amount == 0:
        return array
    return pltpu.roll(array, amount, axis=array.ndim - 1)


def pack_kernel(vec, onsite, intra, codes, inter, field, up_msg, down_msg, left_msg, right_msg):
    for orbital in range(4):
        for block in range(C // LANES):
            cols = slice(block * LANES, (block + 1) * LANES)
            turned = jnp.swapaxes(vec[:, orbital, :, cols], 0, 1)
            for row in range(R):
                field[pl.ds((orbital * R + row) * V, V), cols] = turned[row]
                if row < RIM:
                    up_msg[pl.ds((orbital * RIM + row) * V, V), cols] = turned[row]
                if row >= R - RIM:
                    at = row - (R - RIM)
                    down_msg[pl.ds((orbital * RIM + at) * V, V), cols] = turned[row]

    def plane(index):
        if index < 4:
            return onsite[index]
        if index < 10:
            return intra[(index - 4) // 2, (index - 4) % 2]
        if index < 18:
            return codes[(index - 10) // 2, (index - 10) % 2].astype(jnp.float32)
        return inter[(index - 18) // 2, (index - 18) % 2]

    low = subs_of((R, C)) < 4
    for pair in range(COEFS // 2):
        even, odd = plane(2 * pair), plane(2 * pair + 1)
        odd_turned = pltpu.roll(odd, 4, axis=0)
        rows = pl.ds(FIELD_ROWS + pair * R, R)
        up_msg[rows, :] = jnp.where(low, even, odd_turned)
        down_msg[rows, :] = jnp.where(low, odd_turned, even)

    lane = lanes_of((R, LANES))
    left = jnp.zeros((R, LANES), jnp.float32)
    right = jnp.zeros((R, LANES), jnp.float32)
    for slot in range(32):
        rows = pl.ds(slot * V, V)
        inside = (lane >= 4 * slot) & (lane < 4 * slot + 4)
        left = jnp.where(inside, lane_roll(field[rows, 0:LANES], 4 * slot), left)
        right = jnp.where(inside, lane_roll(field[rows, C - LANES : C], 4 * slot + 4), right)
    left_msg[0:8, :] = left
    right_msg[0:8, :] = right
    left = jnp.zeros((R, LANES), jnp.float32)
    right = jnp.zeros((R, LANES), jnp.float32)
    for slot in range(COEFS):
        values = plane(slot)
        inside = (lane >= 4 * slot) & (lane < 4 * slot + 4)
        left = jnp.where(inside, lane_roll(values[:, 0:LANES], 4 * slot), left)
        right = jnp.where(inside, lane_roll(values[:, C - LANES : C], 4 * slot + 4), right)
    left_msg[8:16, :] = left
    right_msg[8:16, :] = right


def pack(vectors, onsite, intra, codes, inter):
    f32 = jnp.float32
    return pl.pallas_call(
        pack_kernel,
        out_shape=(
            jax.ShapeDtypeStruct((4 * R * V, C), f32),
            jax.ShapeDtypeStruct((ROW_MSG, C), f32),
            jax.ShapeDtypeStruct((ROW_MSG, C), f32),
            jax.ShapeDtypeStruct((16, LANES), f32),
            jax.ShapeDtypeStruct((16, LANES), f32),
        ),
        name="pack",
    )(vectors, onsite, intra, codes, inter)


def table_rows(plane, block, half):
    return pl.ds((block * PLANES + plane) * RING + half * R, R)


def shift_plane(table, source, target, half, amount):
    blocks = range(W // LANES)
    row = jnp.concatenate([table[table_rows(source, block, half), :] for block in blocks], axis=1)
    row = lane_roll(row, amount)
    for block in blocks:
        table[table_rows(target, block, half), :] = row[:, block * LANES : (block + 1) * LANES]


def build_table(onsite, intra, codes, inter, below, above, edge_left, edge_right, table):
    low = subs_of((R, LANES)) < 4
    lane = lanes_of((R, LANES))

    def plane_tile(index, block, half):
        cols = slice(block * LANES, (block + 1) * LANES)
        if block == C // LANES:
            return jnp.where(
                lane < 64,
                lane_roll(edge_right[half], -4 * index),
                lane_roll(edge_left[half], 124 - 4 * index),
            )
        if half == 0:
            if index < 4:
                return onsite[index, :, cols]
            if index < 10:
                return intra[(index - 4) // 2, (index - 4) % 2, :, cols]
            if index < 18:
                return codes[(index - 10) // 2, (index - 10) % 2, :, cols].astype(jnp.float32)
            return inter[(index - 18) // 2, (index - 18) % 2, :, cols]
        rows = pl.ds(FIELD_ROWS + index // 2 * R, R)
        if index % 2 == 0:
            return jnp.where(low, below[rows, cols], above[rows, cols])
        return pltpu.roll(jnp.where(low, above[rows, cols], below[rows, cols]), 4, axis=0)

    for half in range(2):
        def put(plane, block, values):
            table[table_rows(plane, block, half), :] = values

        for block in range(W // LANES):
            for index in range(4):
                put(ONSITE + index, block, 2.0 * plane_tile(index, block, half))
            for index in range(6):
                put(INTRA + index, block, 2.0 * plane_tile(4 + index, block, half))
            for source in range(2):
                marks = [plane_tile(10 + 2 * k + source, block, half) for k in range(4)]
                hops = [2.0 * plane_tile(18 + 2 * k + source, block, half) for k in range(4)]
                for code in range(18):
                    terms = [jnp.where(m == float(code), h, 0.0) for m, h in zip(marks, hops)]
                    put(
                        FWD + source * 18 + code,
                        block,
                        (terms[0] + terms[1]) + (terms[2] + terms[3]),
                    )
        for source in range(2):
            for code in SIDE_CODES:
                shift_plane(
                    table,
                    FWD + source * 18 + code,
                    shifted_plane(source, code),
                    half,
                    offsets(code)[1],
                )
        for layer in range(2):
            shift_plane(table, INTRA + 4 + layer, INTRA_SHIFTED + layer, half, -1)


def field_rows(orbital, row):
    start = (orbital * RING + row) * V
    if not isinstance(start, int):
        start = pl.multiple_of(start, V)
    return pl.ds(start, V)


def put_row(field, orbital, row, values):
    rows = field_rows(orbital, row)
    field[1, rows, :] = values
    field[0, rows, :] = lane_roll(values, 1)
    field[2, rows, :] = lane_roll(values, -1)


def stencil_cell(field, table, row, block):
    cols = slice(block * LANES, (block + 1) * LANES)
    at = [(row - 1) & (RING - 1), row, (row + 1) & (RING - 1)]
    cache = {}

    def value(orbital, row_off, col_off):
        key = (orbital, row_off, col_off)
        if key not in cache:
            cache[key] = field[1 + col_off, field_rows(orbital, at[1 + row_off]), cols]
        return cache[key]

    def coef(plane, row_off):
        return table[pl.ds((block * PLANES + plane) * RING + at[1 + row_off], V, stride=0), :]

    sums = [[None, None] for _ in range(4)]

    def add(orbital, term):
        pair = sums[orbital]
        turn = counts[orbital] % 2
        pair[turn] = term if pair[turn] is None else pair[turn] + term
        counts[orbital] += 1

    counts = [0, 0, 0, 0]
    for layer in range(2):
        a, b = 2 * layer, 2 * layer + 1
        add(a, coef(ONSITE + a, 0) * value(a, 0, 0))
        add(b, coef(ONSITE + b, 0) * value(b, 0, 0))
        straight = coef(INTRA + layer, 0)
        add(a, straight * value(b, 0, 0))
        add(b, straight * value(a, 0, 0))
        add(a, coef(INTRA + 2 + layer, 0) * value(b, -1, 0))
        add(b, coef(INTRA + 2 + layer, 1) * value(a, 1, 0))
        add(a, coef(INTRA + 4 + layer, 0) * value(b, 0, -1))
        add(b, coef(INTRA_SHIFTED + layer, 0) * value(a, 0, 1))
    for code in range(18):
        target = 2 + code // 9
        row_off, col_off = offsets(code)
        for source in range(2):
            add(source, coef(FWD + source * 18 + code, 0) * value(target, row_off, col_off))
            add(
                target,
                coef(shifted_plane(source, code), -row_off) * value(source, -row_off, -col_off),
            )
    return [pair[0] + pair[1] for pair in sums]


def moments_kernel_body(
    first, onsite, intra, codes, inter, below, above, left, right, below_corner, above_corner,
    out, partial, zero, one, two, table, last
):
    blocks = C // LANES
    low = subs_of((R, LANES)) < 4
    lane = lanes_of((R, LANES))
    edge_left = [
        left[8:16, :],
        jnp.where(low, below_corner[8:16, :], above_corner[8:16, :]),
    ]
    edge_right = [
        right[8:16, :],
        jnp.where(low, below_corner[24:32, :], above_corner[24:32, :]),
    ]
    build_table(onsite, intra, codes, inter, below, above, edge_left, edge_right, table)

    for orbital in range(4):
        for row in list(range(R + RIM)) + list(range(RING - RIM, RING)):
            if row < R:
                middle = first[pl.ds((orbital * R + row) * V, V), :]
                sides = (left[0:8, :], right[0:8, :])
            elif row < R + RIM:
                middle = below[pl.ds((orbital * RIM + row - R) * V, V), :]
                sides = (below_corner[0:8, :], below_corner[16:24, :])
            else:
                middle = above[pl.ds((orbital * RIM + row - (RING - RIM)) * V, V), :]
                sides = (above_corner[0:8, :], above_corner[16:24, :])
            slot = orbital * 8 + row % 8
            rim = jnp.where(
                lane < 64, lane_roll(sides[1], -4 * slot), lane_roll(sides[0], 124 - 4 * slot)
            )
            put_row(zero, orbital, row, jnp.concatenate([middle, rim], axis=1))

    def first_row(step, carry):
        row = (step - 2) & (RING - 1)
        results = [stencil_cell(zero, table, row, block) for block in range(W // LANES)]
        for orbital in range(4):
            values = jnp.concatenate([0.5 * r[orbital] for r in results], axis=1)
            put_row(one, orbital, row, values)
        return carry

    lax.fori_loop(0, R + 4, first_row, 0)

    def second_row(step, carry):
        row = (step - 1) & (RING - 1)
        results = [stencil_cell(one, table, row, block) for block in range(W // LANES)]
        for orbital in range(4):
            values = jnp.concatenate([r[orbital] for r in results], axis=1)
            values = values - zero[1, field_rows(orbital, row), :]
            put_row(two, orbital, row, values)
        return carry

    lax.fori_loop(0, R + 2, second_row, 0)

    def third_row(row, sums):
        sums = list(sums)
        for block in range(blocks):
            cols = slice(block * LANES, (block + 1) * LANES)
            result = stencil_cell(two, table, row, block)
            for orbital in range(4):
                rows = field_rows(orbital, row)
                t0 = zero[1, rows, cols]
                t1 = one[1, rows, cols]
                t2 = two[1, rows, cols]
                t3 = result[orbital] - t1
                last[pl.ds(pl.multiple_of((orbital * R + row) * V, V), V), cols] = t3
                for at, (x, y) in enumerate(
                    ((t0, t0), (t1, t0), (t1, t1), (t2, t1), (t2, t2), (t3, t2), (t3, t3))
                ):
                    sums[at] = sums[at] + x * y
        return tuple(sums)

    empty = jnp.zeros((V, LANES), jnp.float32)
    sums = lax.fori_loop(0, R, third_row, (empty,) * 7)

    for orbital in range(4):
        for block in range(blocks):
            cols = slice(block * LANES, (block + 1) * LANES)
            rows = pl.ds(orbital * R * V, R * V)
            turned = jnp.swapaxes(last[rows, cols].reshape(R, V, LANES), 0, 1)
            out[:, orbital, :, cols] = turned

    spread = empty
    sub = subs_of((V, LANES))
    for at in range(7):
        total = jnp.sum(sums[at], axis=1, keepdims=True)
        spread = jnp.where(lane == 8 * at + sub, total, spread)
    line = jnp.sum(spread, axis=0, keepdims=True)
    partial[...] = jnp.broadcast_to(line, partial.shape)


def apply_terms(devices, *args):
    f32 = jnp.float32
    return pl.pallas_call(
        moments_kernel_body,
        out_shape=(
            jax.ShapeDtypeStruct((V, 4, R, C), f32),
            jax.ShapeDtypeStruct((devices, LANES), f32),
        ),
        scratch_shapes=[
            pltpu.VMEM((3, 4 * RING * V, W), f32),
            pltpu.VMEM((3, 4 * RING * V, W), f32),
            pltpu.VMEM((3, 4 * RING * V, W), f32),
            pltpu.VMEM((W // LANES * PLANES * RING, LANES), f32),
            pltpu.VMEM((4 * R * V, C), f32),
        ],
        name="terms",
    )(*args)


def finish_kernel(orbitals, parts, out):
    line = jnp.sum(parts[...], axis=0, keepdims=True) / orbitals
    rows = [lane_roll(line, -8 * at)[:, 0:V] for at in range(7)]
    out[0:1, :] = rows[0]
    out[1:2, :] = rows[1]
    for at in range(2, 7):
        out[at : at + 1, :] = 2.0 * rows[at] - rows[at % 2]


def finish(parts, orbitals):
    return pl.pallas_call(
        functools.partial(finish_kernel, orbitals),
        out_shape=jax.ShapeDtypeStruct((7, V), jnp.float32),
        name="finish",
    )(parts)


def on_device(vectors, onsite, intra_hop, inter_index, inter_hop):
    cols = lax.axis_size("col")
    tiles = lax.axis_size(TILE)
    devices = cols * tiles

    def ring(count, step):
        return [(i, (i + step) % count) for i in range(count)]

    field, up_msg, down_msg, left_msg, right_msg = pack(
        vectors, onsite, intra_hop, inter_index, inter_hop
    )
    below = lax.ppermute(up_msg, TILE, ring(tiles, -1))
    above = lax.ppermute(down_msg, TILE, ring(tiles, 1))
    right = lax.ppermute(left_msg, "col", ring(cols, -1))
    left = lax.ppermute(right_msg, "col", ring(cols, 1))
    corner = jnp.concatenate([left, right], axis=0)
    below_corner = lax.ppermute(corner, TILE, ring(tiles, -1))
    above_corner = lax.ppermute(corner, TILE, ring(tiles, 1))
    last_term, partial = apply_terms(
        devices, field, onsite, intra_hop, inter_index, inter_hop,
        below, above, left, right, below_corner, above_corner,
    )
    parts = lax.all_to_all(partial, EVERY, 0, 0)
    return last_term, finish(parts, 4.0 * R * C * devices)


def solution(mesh):
    torus = Mesh(
        mesh.devices.reshape(mesh.shape["col"], 4, 8, 2), ("col", "tile_0", "tile_1", "tile_2")
    )
    placed = (
        P(None, None, TILE, "col"),
        P(None, TILE, "col"),
        P(None, None, TILE, "col"),
        P(None, None, TILE, "col"),
        P(None, None, TILE, "col"),
    )
    return jax.shard_map(
        on_device,
        mesh=torus,
        in_specs=placed,
        out_specs=(P(None, None, TILE, "col"), P()),
        check_vma=False,
    )
```

```python
import functools

import jax
import jax.numpy as jnp
from jax import lax
from jax.experimental import pallas as pl
from jax.experimental.pallas import tpu as pltpu
from jax.sharding import Mesh
from jax.sharding import PartitionSpec as P

TILE = ("tile_0", "tile_1", "tile_2")
EVERY = ("col",) + TILE

V = 8
R = 8
C = 512
W = C + 128
RING = 16
RIM = 3
COEFS = 26
LANES = 128
BLOCKS = C // LANES
LAST = LANES - 1
STEP = RING + 1
VMEM = pl.BlockSpec(memory_space=pltpu.VMEM)
FIELD_ROWS = 4 * RIM * V
ROW_MSG = FIELD_ROWS + COEFS * 4

FWD = 0
SHIFTED = 36
INTRA = 60
INTRA_SHIFTED = 66
ONSITE = 68
PLANES = 72
STRIDE = PLANES + 1
TABLE = (C // LANES + 1) * RING * STRIDE
FIELD = (3, 4 * STEP * V, W)

SIDE_CODES = [code for code in range(18) if code % 3 != 1]


def offsets(code):
    return code % 9 // 3 - 1, code % 3 - 1


def shifted_plane(source, code):
    if code % 3 == 1:
        return FWD + source * 18 + code
    return SHIFTED + source * 12 + SIDE_CODES.index(code)


def lanes_of(shape):
    return lax.broadcasted_iota(jnp.int32, shape, len(shape) - 1)


def subs_of(shape):
    return lax.broadcasted_iota(jnp.int32, shape, len(shape) - 2)


def lane_roll(array, amount):
    amount = amount % array.shape[-1]
    if amount == 0:
        return array
    return pltpu.roll(array, amount, axis=array.ndim - 1)


def pack_kernel(vec, onsite, intra, codes, inter, field, coefs, up_msg, down_msg, left_msg, right_msg):
    for orbital in range(4):
        for block in range(C // LANES):
            cols = slice(block * LANES, (block + 1) * LANES)
            turned = jnp.swapaxes(vec[:, orbital, :, cols], 0, 1)
            for row in range(R):
                field[pl.ds((orbital * R + row) * V, V), cols] = turned[row]
                if row < RIM:
                    up_msg[pl.ds((orbital * RIM + row) * V, V), cols] = turned[row]
                if row >= R - RIM:
                    at = row - (R - RIM)
                    down_msg[pl.ds((orbital * RIM + at) * V, V), cols] = turned[row]

    def plane(index):
        if index < 4:
            return onsite[index]
        if index < 10:
            return intra[(index - 4) // 2, (index - 4) % 2]
        if index < 18:
            return codes[(index - 10) // 2, (index - 10) % 2].astype(jnp.float32)
        return inter[(index - 18) // 2, (index - 18) % 2]

    for index in range(COEFS):
        coefs[pl.ds(index * R, R), :] = plane(index)

    low = subs_of((R, C)) < 4
    for pair in range(COEFS // 2):
        even, odd = plane(2 * pair), plane(2 * pair + 1)
        odd_turned = pltpu.roll(odd, 4, axis=0)
        rows = pl.ds(FIELD_ROWS + pair * R, R)
        up_msg[rows, :] = jnp.where(low, even, odd_turned)
        down_msg[rows, :] = jnp.where(low, odd_turned, even)

    lane = lanes_of((R, LANES))
    left = jnp.zeros((R, LANES), jnp.float32)
    right = jnp.zeros((R, LANES), jnp.float32)
    for slot in range(32):
        rows = pl.ds(slot * V, V)
        inside = (lane >= 4 * slot) & (lane < 4 * slot + 4)
        left = jnp.where(inside, lane_roll(field[rows, 0:LANES], 4 * slot), left)
        right = jnp.where(inside, lane_roll(field[rows, C - LANES : C], 4 * slot + 4), right)
    left_msg[0:8, :] = left
    right_msg[0:8, :] = right
    left = jnp.zeros((R, LANES), jnp.float32)
    right = jnp.zeros((R, LANES), jnp.float32)
    for slot in range(COEFS):
        values = plane(slot)
        inside = (lane >= 4 * slot) & (lane < 4 * slot + 4)
        left = jnp.where(inside, lane_roll(values[:, 0:LANES], 4 * slot), left)
        right = jnp.where(inside, lane_roll(values[:, C - LANES : C], 4 * slot + 4), right)
    left_msg[8:16, :] = left
    right_msg[8:16, :] = right


def pack(vectors, onsite, intra, codes, inter):
    f32 = jnp.float32
    return pl.pallas_call(
        pack_kernel,
        out_shape=(
            jax.ShapeDtypeStruct((4 * R * V, C), f32),
            jax.ShapeDtypeStruct((COEFS * R, C), f32),
            jax.ShapeDtypeStruct((ROW_MSG, C), f32),
            jax.ShapeDtypeStruct((ROW_MSG, C), f32),
            jax.ShapeDtypeStruct((16, LANES), f32),
            jax.ShapeDtypeStruct((16, LANES), f32),
        ),
        out_specs=(VMEM,) * 6,
        compiler_params=pltpu.CompilerParams(vmem_limit_bytes=65190000),
        name="pack",
    )(vectors, onsite, intra, codes, inter)


def table_rows(plane, block, half):
    return pl.ds((block * RING + half * R) * STRIDE + plane, R, stride=STRIDE)


def planes_of(plane_at):
    kept = {}
    for index in range(4):
        kept[ONSITE + index] = 2.0 * plane_at(index)
    for index in range(6):
        kept[INTRA + index] = 2.0 * plane_at(4 + index)
    for source in range(2):
        marks = [plane_at(10 + 2 * k + source) for k in range(4)]
        hops = [2.0 * plane_at(18 + 2 * k + source) for k in range(4)]
        for code in range(18):
            terms = [jnp.where(m == float(code), h, 0.0) for m, h in zip(marks, hops)]
            kept[FWD + source * 18 + code] = (terms[0] + terms[1]) + (terms[2] + terms[3])
    return kept


def shifts():
    for source in range(2):
        for code in SIDE_CODES:
            yield FWD + source * 18 + code, shifted_plane(source, code), offsets(code)[1]
    for layer in range(2):
        yield INTRA + 4 + layer, INTRA_SHIFTED + layer, -1


def put_half(table, half, plane_at):
    kept = []
    for block in range(BLOCKS):
        kept.append(planes_of(lambda index: plane_at(index, block)))
        for plane, values in kept[-1].items():
            table[table_rows(plane, block, half), :] = values
    for plane, shifted, amount in shifts():
        row = lane_roll(jnp.concatenate([planes[plane] for planes in kept], axis=1), amount)
        for block in range(BLOCKS):
            at = table_rows(shifted, block, half)
            table[at, :] = row[:, block * LANES : (block + 1) * LANES]


def field_rows(orbital, row):
    start = (orbital * STEP + row) * V
    if not isinstance(start, int):
        start = pl.multiple_of(start, V)
    return pl.ds(start, V)


def put_middle(field, orbital, row, values):
    rows = field_rows(orbital, row)
    field[1, rows, 0:C] = values
    field[0, rows, 0:C] = lane_roll(values, 1)
    field[2, rows, 0:C] = lane_roll(values, -1)


def swap_in(amount, rim, turned, lane):
    rolled = lane_roll(rim, amount)
    outer = lane == (0 if amount == 1 else LAST)
    return jnp.where(outer, rolled, turned), jnp.where(outer, turned, rolled)


def own_kernel(first, coefs, zero, table):
    for orbital in range(4):
        for row in range(R):
            put_middle(zero, orbital, row, first[pl.ds((orbital * R + row) * V, V), :])

    def plane_at(index, block):
        return coefs[pl.ds(index * R, R), block * LANES : (block + 1) * LANES]

    put_half(table, 0, plane_at)


def own(field, coefs):
    f32 = jnp.float32
    return pl.pallas_call(
        own_kernel,
        out_shape=(
            jax.ShapeDtypeStruct(FIELD, f32),
            jax.ShapeDtypeStruct((TABLE, LANES), f32),
        ),
        in_specs=[VMEM] * 2,
        out_specs=(VMEM,) * 2,
        compiler_params=pltpu.CompilerParams(vmem_limit_bytes=4 << 20),
        cost_estimate=pl.CostEstimate(flops=4000000, bytes_accessed=4000000, transcendentals=0),
        name="own",
    )(field, coefs)


def near_kernel(zero_in, table_in, below, above, zero, table):
    for orbital in range(4):
        for at in range(RIM):
            rows = pl.ds((orbital * RIM + at) * V, V)
            put_middle(zero, orbital, R + at, below[rows, :])
            put_middle(zero, orbital, RING - RIM + at, above[rows, :])
    low = subs_of((R, LANES)) < 4

    def plane_at(index, block):
        cols = slice(block * LANES, (block + 1) * LANES)
        rows = pl.ds(FIELD_ROWS + index // 2 * R, R)
        if index % 2 == 0:
            return jnp.where(low, below[rows, cols], above[rows, cols])
        return pltpu.roll(jnp.where(low, above[rows, cols], below[rows, cols]), 4, axis=0)

    put_half(table, 1, plane_at)


def near(zero, table, below, above):
    f32 = jnp.float32
    return pl.pallas_call(
        near_kernel,
        out_shape=(
            jax.ShapeDtypeStruct(FIELD, f32),
            jax.ShapeDtypeStruct((TABLE, LANES), f32),
        ),
        in_specs=[VMEM] * 4,
        out_specs=(VMEM,) * 2,
        input_output_aliases={0: 0, 1: 1},
        compiler_params=pltpu.CompilerParams(vmem_limit_bytes=4 << 20),
        cost_estimate=pl.CostEstimate(flops=4000000, bytes_accessed=4000000, transcendentals=0),
        name="near",
    )(zero, table, below, above)


def put_rims(zero, table, left, right, below_corner, above_corner):
    low = subs_of((R, LANES)) < 4
    lane = lanes_of((R, LANES))
    left, right = left[...], right[...]
    below_corner, above_corner = below_corner[...], above_corner[...]

    def rim_of(sides, slot):
        return jnp.where(
            lane < 64, lane_roll(sides[1], -4 * slot), lane_roll(sides[0], 124 - 4 * slot)
        )

    def edges(rows, shift):
        return (
            (left[rows, :], right[rows, :]),
            (below_corner[rows, :], below_corner[shift, :]),
            (above_corner[rows, :], above_corner[shift, :]),
        )

    own_v, below_v, above_v = edges(slice(0, 8), slice(16, 24))
    ring_rows = list(range(R + RIM)) + list(range(RING - RIM, RING))
    for orbital in range(4):
        stores = []
        for row in ring_rows:
            sides = own_v if row < R else below_v if row < R + RIM else above_v
            rim = rim_of(sides, orbital * 8 + row % 8)
            rows = field_rows(orbital, row)
            first_edge, first_rim = swap_in(1, rim, zero[0, rows, 0:LANES], lane)
            last_edge, last_rim = swap_in(-1, rim, zero[2, rows, C - LANES : C], lane)
            stores.append((rows, rim, first_edge, first_rim, last_edge, last_rim))
        for rows, rim, first_edge, first_rim, last_edge, last_rim in stores:
            zero[1, rows, C:W] = rim
            zero[0, rows, 0:LANES] = first_edge
            zero[0, rows, C:W] = first_rim
            zero[2, rows, C - LANES : C] = last_edge
            zero[2, rows, C:W] = last_rim

    own_c, below_c, above_c = edges(slice(8, 16), slice(24, 32))
    near_c = [jnp.where(low, b, a) for b, a in zip(below_c, above_c)]
    stores = []
    for half in range(2):
        rims = [rim_of((own_c, near_c)[half], index) for index in range(COEFS)]
        kept = planes_of(rims.__getitem__)
        for plane, values in kept.items():
            stores.append((table_rows(plane, BLOCKS, half), values))
        for plane, shifted, amount in shifts():
            at = table_rows(shifted, 0 if amount == 1 else BLOCKS - 1, half)
            edge, outer = swap_in(amount, kept[plane], table[at, :], lane)
            stores.append((at, edge))
            stores.append((table_rows(shifted, BLOCKS, half), outer))
    for at, values in stores:
        table[at, :] = values


def stencil_pair(field, table, row, block):
    cols = slice(block * LANES, (block + 1) * LANES)
    at = {step: (row + step) & (RING - 1) for step in range(-1, 3)}
    start = {step: (block * RING + at[step]) * STRIDE for step in at}
    sums = [[None] * 4 for _ in range(2)]

    def add(cell, orbital, plane, step, value):
        coef = table[pl.ds(start[step] + plane, V, stride=0), :]
        term = coef * value
        old = sums[cell][orbital]
        sums[cell][orbital] = term if old is None else old + term

    for step in range(-1, 3):
        for col_off in (-1, 0, 1):
            value = [field[1 + col_off, field_rows(o, at[step]), cols] for o in range(4)]
            for cell in range(2):
                row_off = step - cell
                if abs(row_off) > 1:
                    continue
                code = (row_off + 1) * 3 + col_off + 1
                back = (1 - row_off) * 3 + 1 - col_off
                for source in range(2):
                    for target in range(2):
                        plane = FWD + source * 18 + 9 * target + code
                        add(cell, source, plane, cell, value[2 + target])
                        plane = shifted_plane(source, 9 * target + back)
                        add(cell, 2 + target, plane, step, value[source])
                for layer in range(2):
                    a, b = 2 * layer, 2 * layer + 1
                    if (row_off, col_off) == (0, 0):
                        add(cell, a, ONSITE + a, cell, value[a])
                        add(cell, b, ONSITE + b, cell, value[b])
                        add(cell, a, INTRA + layer, cell, value[b])
                        add(cell, b, INTRA + layer, cell, value[a])
                    elif (row_off, col_off) == (-1, 0):
                        add(cell, a, INTRA + 2 + layer, cell, value[b])
                    elif (row_off, col_off) == (1, 0):
                        add(cell, b, INTRA + 2 + layer, step, value[a])
                    elif (row_off, col_off) == (0, -1):
                        add(cell, a, INTRA + 4 + layer, cell, value[b])
                    elif (row_off, col_off) == (0, 1):
                        add(cell, b, INTRA_SHIFTED + layer, cell, value[a])
    return sums


def term_rows(source, target, table, row, value_of):
    lane = lanes_of((V, LANES))
    count = BLOCKS + 1
    keys = [(cell, orbital) for cell in range(2) for orbital in range(4)]
    rows = {key: field_rows(key[1], (row + key[0]) & (RING - 1)) for key in keys}
    up, down = {}, {}

    def columns(block):
        return slice(block * LANES, (block + 1) * LANES)

    def put_up(block):
        for key in keys:
            inner = up[key, block]
            target[0, rows[key], columns(block)] = jnp.where(
                lane == 0, up[key, (block - 1) % count], inner
            )

    def put_down(block):
        for key in keys:
            inner = down[key, block]
            target[2, rows[key], columns(block)] = jnp.where(
                lane == LAST, down[key, (block + 1) % count], inner
            )

    order = [BLOCKS] + list(range(BLOCKS))
    for at, block in enumerate(order):
        result = stencil_pair(source, table, row, block)
        for key in keys:
            value = value_of(result[key[0]][key[1]], rows[key], columns(block))
            target[1, rows[key], columns(block)] = value
            up[key, block] = lane_roll(value, 1)
            down[key, block] = lane_roll(value, -1)
        if at > 0:
            put_up(block)
            put_down(order[at - 1])
    put_up(order[0])
    put_down(order[-1])


def terms_kernel(
    zero_in, table_in, left, right, below_corner, above_corner,
    out, partial, zero, table, one, two, last
):
    lane = lanes_of((V, LANES))
    put_rims(zero, table, left, right, below_corner, above_corner)

    def first_rows(step, carry):
        row = (2 * step - 2) & (RING - 1)
        term_rows(zero, one, table, row, lambda sum_, rows, cols: 0.5 * sum_)
        return carry

    lax.fori_loop(0, R // 2 + 2, first_rows, 0)

    def second_rows(step, carry):
        row = (2 * step - 1) & (RING - 1)
        term_rows(one, two, table, row, lambda sum_, rows, cols: sum_ - zero[1, rows, cols])
        return carry

    lax.fori_loop(0, R // 2 + 1, second_rows, 0)

    def third_rows(step, sums):
        row = 2 * step
        sums = list(sums)
        for block in range(BLOCKS):
            cols = slice(block * LANES, (block + 1) * LANES)
            result = stencil_pair(two, table, row, block)
            for cell in range(2):
                for orbital in range(4):
                    rows = field_rows(orbital, row + cell)
                    t0 = zero[1, rows, cols]
                    t1 = one[1, rows, cols]
                    t2 = two[1, rows, cols]
                    t3 = result[cell][orbital] - t1
                    at = pl.multiple_of((orbital * R + row + cell) * V, V)
                    last[pl.ds(at, V), cols] = t3
                    for at, (x, y) in enumerate(
                        ((t0, t0), (t1, t0), (t1, t1), (t2, t1), (t2, t2), (t3, t2), (t3, t3))
                    ):
                        sums[at] = sums[at] + x * y
        return tuple(sums)

    empty = jnp.zeros((V, LANES), jnp.float32)
    sums = lax.fori_loop(0, R // 2, third_rows, (empty,) * 7)

    for orbital in range(4):
        for block in range(BLOCKS):
            cols = slice(block * LANES, (block + 1) * LANES)
            rows = pl.ds(orbital * R * V, R * V)
            turned = jnp.swapaxes(last[rows, cols].reshape(R, V, LANES), 0, 1)
            out[:, orbital, :, cols] = turned

    spread = empty
    sub = subs_of((V, LANES))
    for at in range(7):
        total = jnp.sum(sums[at], axis=1, keepdims=True)
        spread = jnp.where(lane == 8 * at + sub, total, spread)
    line = jnp.sum(spread, axis=0, keepdims=True)
    partial[...] = jnp.broadcast_to(line, partial.shape)


def apply_terms(devices, *args):
    f32 = jnp.float32
    results = pl.pallas_call(
        terms_kernel,
        out_shape=(
            jax.ShapeDtypeStruct((V, 4, R, C), f32),
            jax.ShapeDtypeStruct((devices, LANES), f32),
            jax.ShapeDtypeStruct(FIELD, f32),
            jax.ShapeDtypeStruct((TABLE, LANES), f32),
        ),
        in_specs=[VMEM] * 6,
        out_specs=(VMEM,) * 4,
        input_output_aliases={0: 2, 1: 3},
        scratch_shapes=[
            pltpu.VMEM(FIELD, f32),
            pltpu.VMEM(FIELD, f32),
            pltpu.VMEM((4 * R * V, C), f32),
        ],
        compiler_params=pltpu.CompilerParams(vmem_limit_bytes=16 << 20),
        name="terms",
    )(*args)
    return results[0], results[1]


def finish_kernel(orbitals, parts, out):
    line = jnp.sum(parts[...], axis=0, keepdims=True) / orbitals
    rows = [lane_roll(line, -8 * at)[:, 0:V] for at in range(7)]
    out[0:1, :] = rows[0]
    out[1:2, :] = rows[1]
    for at in range(2, 7):
        out[at : at + 1, :] = 2.0 * rows[at] - rows[at % 2]


def finish(parts, orbitals):
    return pl.pallas_call(
        functools.partial(finish_kernel, orbitals),
        out_shape=jax.ShapeDtypeStruct((7, V), jnp.float32),
        in_specs=[VMEM],
        out_specs=VMEM,
        compiler_params=pltpu.CompilerParams(vmem_limit_bytes=1 << 20),
        name="finish",
    )(parts)


def on_device(vectors, onsite, intra_hop, inter_index, inter_hop):
    cols = lax.axis_size("col")
    tiles = lax.axis_size(TILE)
    devices = cols * tiles

    def ring(count, step):
        return [(i, (i + step) % count) for i in range(count)]

    field, coefs, up_msg, down_msg, left_msg, right_msg = pack(
        vectors, onsite, intra_hop, inter_index, inter_hop
    )
    below = lax.ppermute(up_msg, TILE, ring(tiles, -1))
    above = lax.ppermute(down_msg, TILE, ring(tiles, 1))
    right = lax.ppermute(left_msg, "col", ring(cols, -1))
    left = lax.ppermute(right_msg, "col", ring(cols, 1))
    zero, table = own(field, coefs)
    corner = jnp.concatenate([left, right], axis=0)
    below_corner = lax.ppermute(corner, TILE, ring(tiles, -1))
    above_corner = lax.ppermute(corner, TILE, ring(tiles, 1))
    zero, table = near(zero, table, below, above)
    last_term, partial = apply_terms(
        devices, zero, table, left, right, below_corner, above_corner
    )
    parts = lax.all_to_all(partial, EVERY, 0, 0)
    return last_term, finish(parts, 4.0 * R * C * devices)


def solution(mesh):
    torus = Mesh(
        mesh.devices.reshape(mesh.shape["col"], 4, 8, 2), ("col", "tile_0", "tile_1", "tile_2")
    )
    placed = (
        P(None, None, TILE, "col"),
        P(None, TILE, "col"),
        P(None, None, TILE, "col"),
        P(None, None, TILE, "col"),
        P(None, None, TILE, "col"),
    )
    return jax.shard_map(
        on_device,
        mesh=torus,
        in_specs=placed,
        out_specs=(P(None, None, TILE, "col"), P()),
        check_vma=False,
    )
```

```python
import functools

import jax
import jax.numpy as jnp
from jax import lax
from jax.experimental import pallas as pl
from jax.experimental.pallas import tpu as pltpu
from jax.sharding import Mesh
from jax.sharding import PartitionSpec as P


TILE = ("tile_0", "tile_1", "tile_2")
EVERY = ("col",) + TILE

V = 8
R = 8
C = 512
W = C + 128
RING = 16
RIM = 3
COEFS = 26
LANES = 128
BLOCKS = C // LANES
LAST = LANES - 1
STEP = RING + 1
VMEM = pl.BlockSpec(memory_space=pltpu.VMEM)
FIELD_ROWS = 4 * RIM * V
ROW_MSG = FIELD_ROWS + COEFS * 4

FWD = 0
SHIFTED = 36
INTRA = 60
INTRA_SHIFTED = 66
ONSITE = 68
PLANES = 72
STRIDE = PLANES + 1
TABLE = (C // LANES + 1) * RING * STRIDE
FIELD = (3, 4 * STEP * V, W)

SIDE_CODES = [code for code in range(18) if code % 3 != 1]


def offsets(code):
    return code % 9 // 3 - 1, code % 3 - 1


def shifted_plane(source, code):
    if code % 3 == 1:
        return FWD + source * 18 + code
    return SHIFTED + source * 12 + SIDE_CODES.index(code)


def lanes_of(shape):
    return lax.broadcasted_iota(jnp.int32, shape, len(shape) - 1)


def subs_of(shape):
    return lax.broadcasted_iota(jnp.int32, shape, len(shape) - 2)


def lane_roll(array, amount):
    amount = amount % array.shape[-1]
    if amount == 0:
        return array
    return pltpu.roll(array, amount, axis=array.ndim - 1)


def pack_kernel(vec, onsite, intra, codes, inter, field, coefs, up_msg, down_msg, edge_msg):
    for orbital in range(4):
        for block in range(C // LANES):
            cols = slice(block * LANES, (block + 1) * LANES)
            turned = jnp.swapaxes(vec[:, orbital, :, cols], 0, 1)
            for row in range(R):
                field[pl.ds((orbital * R + row) * V, V), cols] = turned[row]
                if row < RIM:
                    up_msg[pl.ds((orbital * RIM + row) * V, V), cols] = turned[row]
                if row >= R - RIM:
                    at = row - (R - RIM)
                    down_msg[pl.ds((orbital * RIM + at) * V, V), cols] = turned[row]

    def plane(index):
        if index < 4:
            return onsite[index]
        if index < 10:
            return intra[(index - 4) // 2, (index - 4) % 2]
        if index < 18:
            return codes[(index - 10) // 2, (index - 10) % 2].astype(jnp.float32)
        return inter[(index - 18) // 2, (index - 18) % 2]

    for index in range(COEFS):
        coefs[pl.ds(index * R, R), :] = plane(index)

    low = subs_of((R, C)) < 4
    for pair in range(COEFS // 2):
        even, odd = plane(2 * pair), plane(2 * pair + 1)
        odd_turned = pltpu.roll(odd, 4, axis=0)
        rows = pl.ds(FIELD_ROWS + pair * R, R)
        up_msg[rows, :] = jnp.where(low, even, odd_turned)
        down_msg[rows, :] = jnp.where(low, odd_turned, even)

    lane = lanes_of((R, LANES))

    def pack_edges(count, block_of):
        packed = [jnp.zeros((R, LANES), jnp.float32) for _ in range(2)]
        for slot in range(count):
            ends = jnp.where(lane < 64, block_of(slot, 0), block_of(slot, C - LANES))
            inside = ((lane + 4) & LAST) >> 3 == slot % 16
            packed[slot // 16] = jnp.where(
                inside, lane_roll(ends, 8 * slot), packed[slot // 16]
            )
        return packed

    packed = pack_edges(32, lambda slot, at: field[pl.ds(slot * V, V), at : at + LANES])
    packed += pack_edges(COEFS, lambda slot, at: coefs[pl.ds(slot * R, R), at : at + LANES])
    for at, values in enumerate(packed):
        edge_msg[at * 8 : at * 8 + 8, :] = values


def pack(vectors, onsite, intra, codes, inter):
    f32 = jnp.float32
    return pl.pallas_call(
        pack_kernel,
        out_shape=(
            jax.ShapeDtypeStruct((4 * R * V, C), f32),
            jax.ShapeDtypeStruct((COEFS * R, C), f32),
            jax.ShapeDtypeStruct((ROW_MSG, C), f32),
            jax.ShapeDtypeStruct((ROW_MSG, C), f32),
            jax.ShapeDtypeStruct((32, LANES), f32),
        ),
        out_specs=(VMEM,) * 5,
        compiler_params=pltpu.CompilerParams(vmem_limit_bytes=16 << 20),
        name="pack",
    )(
        *(
            pltpu.with_memory_space_constraint(array, pltpu.HBM)
            for array in (vectors, onsite, intra, codes, inter)
        )
    )


def table_rows(plane, block, half):
    return pl.ds((block * RING + half * R) * STRIDE + plane, R, stride=STRIDE)


def planes_of(plane_at):
    kept = {}
    for index in range(4):
        kept[ONSITE + index] = 2.0 * plane_at(index)
    for index in range(6):
        kept[INTRA + index] = 2.0 * plane_at(4 + index)
    for source in range(2):
        marks = [plane_at(10 + 2 * k + source) for k in range(4)]
        hops = [2.0 * plane_at(18 + 2 * k + source) for k in range(4)]
        for code in range(18):
            terms = [jnp.where(m == float(code), h, 0.0) for m, h in zip(marks, hops)]
            kept[FWD + source * 18 + code] = (terms[0] + terms[1]) + (terms[2] + terms[3])
    return kept


def shifts():
    for source in range(2):
        for code in SIDE_CODES:
            yield FWD + source * 18 + code, shifted_plane(source, code), offsets(code)[1]
    for layer in range(2):
        yield INTRA + 4 + layer, INTRA_SHIFTED + layer, -1


def put_half(table, half, plane_at):
    kept = []
    for block in range(BLOCKS):
        kept.append(planes_of(lambda index: plane_at(index, block)))
        for plane, values in kept[-1].items():
            table[table_rows(plane, block, half), :] = values
    for plane, shifted, amount in shifts():
        row = lane_roll(jnp.concatenate([planes[plane] for planes in kept], axis=1), amount)
        for block in range(BLOCKS):
            at = table_rows(shifted, block, half)
            table[at, :] = row[:, block * LANES : (block + 1) * LANES]


def field_rows(orbital, row):
    start = (orbital * STEP + row) * V
    if not isinstance(start, int):
        start = pl.multiple_of(start, V)
    return pl.ds(start, V)


def put_middle(field, orbital, row, values):
    rows = field_rows(orbital, row)
    field[1, rows, 0:C] = values
    field[0, rows, 0:C] = lane_roll(values, 1)
    field[2, rows, 0:C] = lane_roll(values, -1)


def swap_in(amount, rolled, turned, lane):
    outer = lane == (0 if amount == 1 else LAST)
    return jnp.where(outer, rolled, turned), jnp.where(outer, turned, rolled)


def own_kernel(first, coefs, zero, table):
    for orbital in range(4):
        for row in range(R):
            put_middle(zero, orbital, row, first[pl.ds((orbital * R + row) * V, V), :])

    def plane_at(index, block):
        return coefs[pl.ds(index * R, R), block * LANES : (block + 1) * LANES]

    put_half(table, 0, plane_at)


def own(field, coefs):
    f32 = jnp.float32
    return pl.pallas_call(
        own_kernel,
        out_shape=(
            jax.ShapeDtypeStruct(FIELD, f32),
            jax.ShapeDtypeStruct((TABLE, LANES), f32),
        ),
        in_specs=[VMEM] * 2,
        out_specs=(VMEM,) * 2,
        compiler_params=pltpu.CompilerParams(vmem_limit_bytes=4 << 20),
        cost_estimate=pl.CostEstimate(flops=4000000, bytes_accessed=4000000, transcendentals=0),
        name="own",
    )(field, coefs)


def near_kernel(zero_in, table_in, below, above, zero, table):
    for orbital in range(4):
        for at in range(RIM):
            rows = pl.ds((orbital * RIM + at) * V, V)
            put_middle(zero, orbital, R + at, below[rows, :])
            put_middle(zero, orbital, RING - RIM + at, above[rows, :])
    low = subs_of((R, LANES)) < 4

    def plane_at(index, block):
        cols = slice(block * LANES, (block + 1) * LANES)
        rows = pl.ds(FIELD_ROWS + index // 2 * R, R)
        if index % 2 == 0:
            return jnp.where(low, below[rows, cols], above[rows, cols])
        return pltpu.roll(jnp.where(low, above[rows, cols], below[rows, cols]), 4, axis=0)

    put_half(table, 1, plane_at)


def near(zero, table, below, above):
    f32 = jnp.float32
    return pl.pallas_call(
        near_kernel,
        out_shape=(
            jax.ShapeDtypeStruct(FIELD, f32),
            jax.ShapeDtypeStruct((TABLE, LANES), f32),
        ),
        in_specs=[VMEM] * 4,
        out_specs=(VMEM,) * 2,
        input_output_aliases={0: 0, 1: 1},
        compiler_params=pltpu.CompilerParams(vmem_limit_bytes=4 << 20),
        cost_estimate=pl.CostEstimate(flops=4000000, bytes_accessed=4000000, transcendentals=0),
        name="near",
    )(zero, table, below, above)


def put_field_rims(zero, edges, ring_rows):
    lane = lanes_of((V, LANES))
    for orbital in range(4):
        stores = []
        for row in ring_rows:
            slot = orbital * 8 + row % 8
            rims = [lane_roll(edges[slot // 16], amount - 8 * slot) for amount in (1, 0, -1)]
            rows = field_rows(orbital, row)
            first = swap_in(1, rims[0], zero[0, rows, 0:LANES], lane)
            last = swap_in(-1, rims[2], zero[2, rows, C - LANES : C], lane)
            stores.append((rows, rims[1], first, last))
        for rows, rim, first, last in stores:
            zero[1, rows, C:W] = rim
            zero[0, rows, 0:LANES], zero[0, rows, C:W] = first
            zero[2, rows, C - LANES : C], zero[2, rows, C:W] = last


def put_table_rims(table, edges, half):
    lane = lanes_of((R, LANES))

    def rolled_by(amount):
        return lambda index: lane_roll(edges[index // 16], amount - 8 * index)

    for plane, values in planes_of(rolled_by(0)).items():
        table[table_rows(plane, BLOCKS, half), :] = values
    for amount in (1, -1):
        rolled = planes_of(rolled_by(amount))
        for plane, shifted, by in shifts():
            if by == amount:
                at = table_rows(shifted, 0 if amount == 1 else BLOCKS - 1, half)
                edge, outer = swap_in(amount, rolled[plane], table[at, :], lane)
                table[at, :] = edge
                table[table_rows(shifted, BLOCKS, half), :] = outer


def put_rims(zero, table, own_edge, below_edge, above_edge):
    low = subs_of((R, LANES)) < 4
    own, below, above = [
        [ref[8 * at : 8 * at + 8, :] for at in range(4)]
        for ref in (own_edge, below_edge, above_edge)
    ]
    put_field_rims(zero, own[:2], range(R))
    put_field_rims(zero, below[:2], range(R, R + RIM))
    put_field_rims(zero, above[:2], range(RING - RIM, RING))
    put_table_rims(table, own[2:], 0)
    put_table_rims(table, [jnp.where(low, b, a) for b, a in zip(below[2:], above[2:])], 1)


def stencil_pair(field, table, row, block):
    cols = slice(block * LANES, (block + 1) * LANES)
    at = {step: (row + step) & (RING - 1) for step in range(-1, 3)}
    start = {step: (block * RING + at[step]) * STRIDE for step in at}
    sums = [[None] * 4 for _ in range(2)]

    def add(cell, orbital, plane, step, value):
        coef = table[pl.ds(start[step] + plane, V, stride=0), :]
        term = coef * value
        old = sums[cell][orbital]
        sums[cell][orbital] = term if old is None else old + term

    for step in range(-1, 3):
        for col_off in (-1, 0, 1):
            value = [field[1 + col_off, field_rows(o, at[step]), cols] for o in range(4)]
            for cell in range(2):
                row_off = step - cell
                if abs(row_off) > 1:
                    continue
                code = (row_off + 1) * 3 + col_off + 1
                back = (1 - row_off) * 3 + 1 - col_off
                for source in range(2):
                    for target in range(2):
                        plane = FWD + source * 18 + 9 * target + code
                        add(cell, source, plane, cell, value[2 + target])
                        plane = shifted_plane(source, 9 * target + back)
                        add(cell, 2 + target, plane, step, value[source])
                for layer in range(2):
                    a, b = 2 * layer, 2 * layer + 1
                    if (row_off, col_off) == (0, 0):
                        add(cell, a, ONSITE + a, cell, value[a])
                        add(cell, b, ONSITE + b, cell, value[b])
                        add(cell, a, INTRA + layer, cell, value[b])
                        add(cell, b, INTRA + layer, cell, value[a])
                    elif (row_off, col_off) == (-1, 0):
                        add(cell, a, INTRA + 2 + layer, cell, value[b])
                    elif (row_off, col_off) == (1, 0):
                        add(cell, b, INTRA + 2 + layer, step, value[a])
                    elif (row_off, col_off) == (0, -1):
                        add(cell, a, INTRA + 4 + layer, cell, value[b])
                    elif (row_off, col_off) == (0, 1):
                        add(cell, b, INTRA_SHIFTED + layer, cell, value[a])
    return sums


def term_rows(source, target, table, row, value_of):
    lane = lanes_of((V, LANES))
    count = BLOCKS + 1
    keys = [(cell, orbital) for cell in range(2) for orbital in range(4)]
    rows = {key: field_rows(key[1], (row + key[0]) & (RING - 1)) for key in keys}
    up, down = {}, {}

    def columns(block):
        return slice(block * LANES, (block + 1) * LANES)

    def put_up(block):
        for key in keys:
            inner = up[key, block]
            target[0, rows[key], columns(block)] = jnp.where(
                lane == 0, up[key, (block - 1) % count], inner
            )

    def put_down(block):
        for key in keys:
            inner = down[key, block]
            target[2, rows[key], columns(block)] = jnp.where(
                lane == LAST, down[key, (block + 1) % count], inner
            )

    order = [BLOCKS] + list(range(BLOCKS))
    for at, block in enumerate(order):
        result = stencil_pair(source, table, row, block)
        for key in keys:
            value = value_of(result[key[0]][key[1]], rows[key], columns(block))
            target[1, rows[key], columns(block)] = value
            up[key, block] = lane_roll(value, 1)
            down[key, block] = lane_roll(value, -1)
        if at > 0:
            put_up(block)
            put_down(order[at - 1])
    put_up(order[0])
    put_down(order[-1])


def terms_kernel(
    zero_in, table_in, own_edge, below_edge, above_edge,
    out, partial, zero, table, one, two, last
):
    lane = lanes_of((V, LANES))
    put_rims(zero, table, own_edge, below_edge, above_edge)

    def first_rows(step, carry):
        row = (2 * step - 2) & (RING - 1)
        term_rows(zero, one, table, row, lambda sum_, rows, cols: 0.5 * sum_)
        return carry

    lax.fori_loop(0, R // 2 + 2, first_rows, 0)

    def second_rows(step, carry):
        row = (2 * step - 1) & (RING - 1)
        term_rows(one, two, table, row, lambda sum_, rows, cols: sum_ - zero[1, rows, cols])
        return carry

    lax.fori_loop(0, R // 2 + 1, second_rows, 0)

    def third_rows(step, sums):
        row = 2 * step
        sums = list(sums)
        for block in range(BLOCKS):
            cols = slice(block * LANES, (block + 1) * LANES)
            result = stencil_pair(two, table, row, block)
            for cell in range(2):
                for orbital in range(4):
                    rows = field_rows(orbital, row + cell)
                    t0 = zero[1, rows, cols]
                    t1 = one[1, rows, cols]
                    t2 = two[1, rows, cols]
                    t3 = result[cell][orbital] - t1
                    at = pl.multiple_of((orbital * R + row + cell) * V, V)
                    last[pl.ds(at, V), cols] = t3
                    for at, (x, y) in enumerate(
                        ((t0, t0), (t1, t0), (t1, t1), (t2, t1), (t2, t2), (t3, t2), (t3, t3))
                    ):
                        sums[at] = sums[at] + x * y
        return tuple(sums)

    empty = jnp.zeros((V, LANES), jnp.float32)
    sums = lax.fori_loop(0, R // 2, third_rows, (empty,) * 7)

    for orbital in range(4):
        for block in range(BLOCKS):
            cols = slice(block * LANES, (block + 1) * LANES)
            rows = pl.ds(orbital * R * V, R * V)
            turned = jnp.swapaxes(last[rows, cols].reshape(R, V, LANES), 0, 1)
            out[:, orbital, :, cols] = turned

    spread = empty
    sub = subs_of((V, LANES))
    for at in range(7):
        total = jnp.sum(sums[at], axis=1, keepdims=True)
        spread = jnp.where(lane == 8 * at + sub, total, spread)
    line = jnp.sum(spread, axis=0, keepdims=True)
    partial[...] = jnp.broadcast_to(line, partial.shape)


def apply_terms(devices, *args):
    f32 = jnp.float32
    results = pl.pallas_call(
        terms_kernel,
        out_shape=(
            jax.ShapeDtypeStruct((V, 4, R, C), f32),
            jax.ShapeDtypeStruct((devices, LANES), f32),
            jax.ShapeDtypeStruct(FIELD, f32),
            jax.ShapeDtypeStruct((TABLE, LANES), f32),
        ),
        in_specs=[VMEM] * 5,
        out_specs=(VMEM,) * 4,
        input_output_aliases={0: 2, 1: 3},
        scratch_shapes=[
            pltpu.VMEM(FIELD, f32),
            pltpu.VMEM(FIELD, f32),
            pltpu.VMEM((4 * R * V, C), f32),
        ],
        compiler_params=pltpu.CompilerParams(vmem_limit_bytes=16 << 20),
        name="terms",
    )(*args)
    return results[0], results[1]


def finish_kernel(orbitals, parts, out):
    line = jnp.sum(parts[...], axis=0, keepdims=True) / orbitals
    rows = [lane_roll(line, -8 * at)[:, 0:V] for at in range(7)]
    out[0:1, :] = rows[0]
    out[1:2, :] = rows[1]
    for at in range(2, 7):
        out[at : at + 1, :] = 2.0 * rows[at] - rows[at % 2]


def finish(parts, orbitals):
    return pl.pallas_call(
        functools.partial(finish_kernel, orbitals),
        out_shape=jax.ShapeDtypeStruct((7, V), jnp.float32),
        in_specs=[VMEM],
        out_specs=VMEM,
        compiler_params=pltpu.CompilerParams(vmem_limit_bytes=1 << 20),
        name="finish",
    )(parts)


def on_device(vectors, onsite, intra_hop, inter_index, inter_hop):
    cols = lax.axis_size("col")
    tiles = lax.axis_size(TILE)
    devices = cols * tiles

    def ring(count, step):
        return [(i, (i + step) % count) for i in range(count)]

    field, coefs, up_msg, down_msg, edge_msg = pack(
        vectors, onsite, intra_hop, inter_index, inter_hop
    )
    right = lax.ppermute(edge_msg, "col", ring(cols, -1))
    left = lax.ppermute(edge_msg, "col", ring(cols, 1))
    below = lax.ppermute(up_msg, TILE, ring(tiles, -1))
    above = lax.ppermute(down_msg, TILE, ring(tiles, 1))
    zero, table = own(field, coefs)
    edge = jnp.where((lanes_of(edge_msg.shape) & 7) < 4, right, left)
    below_edge = lax.ppermute(edge, TILE, ring(tiles, -1))
    above_edge = lax.ppermute(edge, TILE, ring(tiles, 1))
    zero, table = near(zero, table, below, above)
    last_term, partial = apply_terms(devices, zero, table, edge, below_edge, above_edge)
    parts = lax.all_to_all(partial, EVERY, 0, 0)
    return last_term, finish(parts, 4.0 * R * C * devices)


def solution(mesh):
    torus = Mesh(
        mesh.devices.reshape(mesh.shape["col"], 4, 8, 2), ("col", "tile_0", "tile_1", "tile_2")
    )
    placed = (
        P(None, None, TILE, "col"),
        P(None, TILE, "col"),
        P(None, None, TILE, "col"),
        P(None, None, TILE, "col"),
        P(None, None, TILE, "col"),
    )
    return jax.shard_map(
        on_device,
        mesh=torus,
        in_specs=placed,
        out_specs=(P(None, None, TILE, "col"), P()),
        check_vma=False,
    )
```

```python
import functools

import jax
import jax.numpy as jnp
from jax import lax
from jax.experimental import pallas as pl
from jax.experimental.pallas import tpu as pltpu
from jax.sharding import Mesh
from jax.sharding import PartitionSpec as P


TILE = ("tile_0", "tile_1", "tile_2")
EVERY = ("col",) + TILE

V = 8
R = 8
C = 512
W = C + 128
RING = 16
RIM = 3
COEFS = 26
LANES = 128
BLOCKS = C // LANES
LAST = LANES - 1
STEP = RING + 1
VMEM = pl.BlockSpec(memory_space=pltpu.VMEM)
FIELD_ROWS = 4 * RIM * V
TURNED = COEFS // R
PAIR_ROWS = FIELD_ROWS + TURNED * RIM * R
ROW_MSG = PAIR_ROWS + (COEFS - TURNED * R) * 4

FWD = 0
SHIFTED = 36
INTRA = 60
INTRA_SHIFTED = 66
ONSITE = 68
PLANES = 72
STRIDE = PLANES + 1
TABLE = (C // LANES + 1) * RING * STRIDE
FIELD = (3, 4 * STEP * V, W)

SIDE_CODES = [code for code in range(18) if code % 3 != 1]


def offsets(code):
    return code % 9 // 3 - 1, code % 3 - 1


def shifted_plane(source, code):
    if code % 3 == 1:
        return FWD + source * 18 + code
    return SHIFTED + source * 12 + SIDE_CODES.index(code)


def lanes_of(shape):
    return lax.broadcasted_iota(jnp.int32, shape, len(shape) - 1)


def subs_of(shape):
    return lax.broadcasted_iota(jnp.int32, shape, len(shape) - 2)


def lane_roll(array, amount):
    amount = amount % array.shape[-1]
    if amount == 0:
        return array
    return pltpu.roll(array, amount, axis=array.ndim - 1)


def pack_kernel(vec, onsite, intra, codes, inter, field, coefs, up_msg, down_msg, edge_msg):
    for orbital in range(4):
        for block in range(C // LANES):
            cols = slice(block * LANES, (block + 1) * LANES)
            turned = jnp.swapaxes(vec[:, orbital, :, cols], 0, 1)
            for row in range(R):
                field[pl.ds((orbital * R + row) * V, V), cols] = turned[row]
                if row < RIM:
                    up_msg[pl.ds((orbital * RIM + row) * V, V), cols] = turned[row]
                if row >= R - RIM:
                    at = row - (R - RIM)
                    down_msg[pl.ds((orbital * RIM + at) * V, V), cols] = turned[row]

    def plane(index):
        if index < 4:
            return onsite[index]
        if index < 10:
            return intra[(index - 4) // 2, (index - 4) % 2]
        if index < 18:
            return codes[(index - 10) // 2, (index - 10) % 2].astype(jnp.float32)
        return inter[(index - 18) // 2, (index - 18) % 2]

    for index in range(COEFS):
        coefs[pl.ds(index * R, R), :] = plane(index)

    for group in range(TURNED):
        for block in range(BLOCKS):
            cols = slice(block * LANES, (block + 1) * LANES)
            values = coefs[pl.ds(group * R * R, R * R), cols].reshape(R, R, LANES)
            turned = jnp.swapaxes(values, 0, 1)
            for at in range(RIM):
                rows = pl.ds(FIELD_ROWS + (group * RIM + at) * R, R)
                up_msg[rows, cols] = turned[at]
                down_msg[rows, cols] = turned[R - RIM + at]
    low = subs_of((R, C)) < 4
    even, odd = plane(COEFS - 2), pltpu.roll(plane(COEFS - 1), 4, axis=0)
    up_msg[pl.ds(PAIR_ROWS, R), :] = jnp.where(low, even, odd)
    down_msg[pl.ds(PAIR_ROWS, R), :] = jnp.where(low, odd, even)

    lane = lanes_of((R, LANES))

    def pack_edges(count, block_of):
        packed = [jnp.zeros((R, LANES), jnp.float32) for _ in range(2)]
        for slot in range(count):
            ends = jnp.where(lane < 64, block_of(slot, 0), block_of(slot, C - LANES))
            inside = ((lane + 4) & LAST) >> 3 == slot % 16
            packed[slot // 16] = jnp.where(
                inside, lane_roll(ends, 8 * slot), packed[slot // 16]
            )
        return packed

    packed = pack_edges(32, lambda slot, at: field[pl.ds(slot * V, V), at : at + LANES])
    packed += pack_edges(COEFS, lambda slot, at: coefs[pl.ds(slot * R, R), at : at + LANES])
    for at, values in enumerate(packed):
        edge_msg[at * 8 : at * 8 + 8, :] = values


def pack(vectors, onsite, intra, codes, inter):
    f32 = jnp.float32
    return pl.pallas_call(
        pack_kernel,
        out_shape=(
            jax.ShapeDtypeStruct((4 * R * V, C), f32),
            jax.ShapeDtypeStruct((COEFS * R, C), f32),
            jax.ShapeDtypeStruct((ROW_MSG, C), f32),
            jax.ShapeDtypeStruct((ROW_MSG, C), f32),
            jax.ShapeDtypeStruct((32, LANES), f32),
        ),
        out_specs=(VMEM,) * 5,
        compiler_params=pltpu.CompilerParams(vmem_limit_bytes=16 << 20),
        name="pack",
    )(
        *(
            pltpu.with_memory_space_constraint(array, pltpu.HBM)
            for array in (vectors, onsite, intra, codes, inter)
        )
    )


def table_rows(plane, block, half):
    return pl.ds((block * RING + half * R) * STRIDE + plane, R, stride=STRIDE)


def planes_of(plane_at):
    kept = {}
    for index in range(4):
        kept[ONSITE + index] = 2.0 * plane_at(index)
    for index in range(6):
        kept[INTRA + index] = 2.0 * plane_at(4 + index)
    for source in range(2):
        marks = [plane_at(10 + 2 * k + source) for k in range(4)]
        hops = [2.0 * plane_at(18 + 2 * k + source) for k in range(4)]
        for code in range(18):
            terms = [jnp.where(m == float(code), h, 0.0) for m, h in zip(marks, hops)]
            kept[FWD + source * 18 + code] = (terms[0] + terms[1]) + (terms[2] + terms[3])
    return kept


def shifts():
    for source in range(2):
        for code in SIDE_CODES:
            yield FWD + source * 18 + code, shifted_plane(source, code), offsets(code)[1]
    for layer in range(2):
        yield INTRA + 4 + layer, INTRA_SHIFTED + layer, -1


def put_half(table, half, plane_at):
    kept = []
    for block in range(BLOCKS):
        kept.append(planes_of(lambda index: plane_at(index, block)))
        for plane, values in kept[-1].items():
            table[table_rows(plane, block, half), :] = values
    for plane, shifted, amount in shifts():
        row = lane_roll(jnp.concatenate([planes[plane] for planes in kept], axis=1), amount)
        for block in range(BLOCKS):
            at = table_rows(shifted, block, half)
            table[at, :] = row[:, block * LANES : (block + 1) * LANES]


def field_rows(orbital, row):
    start = (orbital * STEP + row) * V
    if not isinstance(start, int):
        start = pl.multiple_of(start, V)
    return pl.ds(start, V)


def put_middle(field, orbital, row, values):
    rows = field_rows(orbital, row)
    field[1, rows, 0:C] = values
    field[0, rows, 0:C] = lane_roll(values, 1)
    field[2, rows, 0:C] = lane_roll(values, -1)


def swap_in(amount, rolled, turned, lane):
    outer = lane == (0 if amount == 1 else LAST)
    return jnp.where(outer, rolled, turned), jnp.where(outer, turned, rolled)


def own_kernel(first, coefs, zero, table):
    for orbital in range(4):
        for row in range(R):
            put_middle(zero, orbital, row, first[pl.ds((orbital * R + row) * V, V), :])

    def plane_at(index, block):
        return coefs[pl.ds(index * R, R), block * LANES : (block + 1) * LANES]

    put_half(table, 0, plane_at)


def own(field, coefs):
    f32 = jnp.float32
    return pl.pallas_call(
        own_kernel,
        out_shape=(
            jax.ShapeDtypeStruct(FIELD, f32),
            jax.ShapeDtypeStruct((TABLE, LANES), f32),
        ),
        in_specs=[VMEM] * 2,
        out_specs=(VMEM,) * 2,
        compiler_params=pltpu.CompilerParams(vmem_limit_bytes=4 << 20),
        cost_estimate=pl.CostEstimate(flops=4000000, bytes_accessed=4000000, transcendentals=0),
        name="own",
    )(field, coefs)


def near_kernel(zero_in, table_in, below, above, zero, table):
    for orbital in range(4):
        for at in range(RIM):
            rows = pl.ds((orbital * RIM + at) * V, V)
            put_middle(zero, orbital, R + at, below[rows, :])
            put_middle(zero, orbital, RING - RIM + at, above[rows, :])
    low = subs_of((R, LANES)) < 4
    turned = {}
    for group in range(TURNED):
        for block in range(BLOCKS):
            cols = slice(block * LANES, (block + 1) * LANES)
            rows = [pl.ds(FIELD_ROWS + (group * RIM + at) * R, R) for at in range(RIM)]
            first = [below[at, cols] for at in rows]
            last = [above[at, cols] for at in rows]
            values = jnp.stack(first + [first[-1], last[0]] + last)
            turned[group, block] = jnp.swapaxes(values, 0, 1)

    def plane_at(index, block):
        if index < TURNED * R:
            return turned[index // R, block][index % R]
        cols = slice(block * LANES, (block + 1) * LANES)
        rows = pl.ds(PAIR_ROWS, R)
        if index % 2 == 0:
            return jnp.where(low, below[rows, cols], above[rows, cols])
        return pltpu.roll(jnp.where(low, above[rows, cols], below[rows, cols]), 4, axis=0)

    put_half(table, 1, plane_at)


def near(zero, table, below, above):
    f32 = jnp.float32
    return pl.pallas_call(
        near_kernel,
        out_shape=(
            jax.ShapeDtypeStruct(FIELD, f32),
            jax.ShapeDtypeStruct((TABLE, LANES), f32),
        ),
        in_specs=[VMEM] * 4,
        out_specs=(VMEM,) * 2,
        input_output_aliases={0: 0, 1: 1},
        compiler_params=pltpu.CompilerParams(vmem_limit_bytes=4 << 20),
        cost_estimate=pl.CostEstimate(flops=4000000, bytes_accessed=4000000, transcendentals=0),
        name="near",
    )(zero, table, below, above)


def put_field_rims(zero, edges, ring_rows):
    lane = lanes_of((V, LANES))
    for orbital in range(4):
        stores = []
        for row in ring_rows:
            slot = orbital * 8 + row % 8
            rims = [lane_roll(edges[slot // 16], amount - 8 * slot) for amount in (1, 0, -1)]
            rows = field_rows(orbital, row)
            first = swap_in(1, rims[0], zero[0, rows, 0:LANES], lane)
            last = swap_in(-1, rims[2], zero[2, rows, C - LANES : C], lane)
            stores.append((rows, rims[1], first, last))
        for rows, rim, first, last in stores:
            zero[1, rows, C:W] = rim
            zero[0, rows, 0:LANES], zero[0, rows, C:W] = first
            zero[2, rows, C - LANES : C], zero[2, rows, C:W] = last


def put_table_rims(table, edges, half):
    lane = lanes_of((R, LANES))

    def rolled_by(amount):
        return lambda index: lane_roll(edges[index // 16], amount - 8 * index)

    for plane, values in planes_of(rolled_by(0)).items():
        table[table_rows(plane, BLOCKS, half), :] = values
    for amount in (1, -1):
        rolled = planes_of(rolled_by(amount))
        for plane, shifted, by in shifts():
            if by == amount:
                at = table_rows(shifted, 0 if amount == 1 else BLOCKS - 1, half)
                edge, outer = swap_in(amount, rolled[plane], table[at, :], lane)
                table[at, :] = edge
                table[table_rows(shifted, BLOCKS, half), :] = outer


def registers(edge):
    return [edge[8 * at : 8 * at + 8, :] for at in range(4)]


def stencil_pair(field, table, row, block):
    cols = slice(block * LANES, (block + 1) * LANES)
    at = {step: (row + step) & (RING - 1) for step in range(-1, 3)}
    start = {step: (block * RING + at[step]) * STRIDE for step in at}
    sums = [[None] * 4 for _ in range(2)]

    def add(cell, orbital, plane, step, value):
        coef = table[pl.ds(start[step] + plane, V, stride=0), :]
        term = coef * value
        old = sums[cell][orbital]
        sums[cell][orbital] = term if old is None else old + term

    for step in range(-1, 3):
        for col_off in (-1, 0, 1):
            value = [field[1 + col_off, field_rows(o, at[step]), cols] for o in range(4)]
            for cell in range(2):
                row_off = step - cell
                if abs(row_off) > 1:
                    continue
                code = (row_off + 1) * 3 + col_off + 1
                back = (1 - row_off) * 3 + 1 - col_off
                for source in range(2):
                    for target in range(2):
                        plane = FWD + source * 18 + 9 * target + code
                        add(cell, source, plane, cell, value[2 + target])
                        plane = shifted_plane(source, 9 * target + back)
                        add(cell, 2 + target, plane, step, value[source])
                for layer in range(2):
                    a, b = 2 * layer, 2 * layer + 1
                    if (row_off, col_off) == (0, 0):
                        add(cell, a, ONSITE + a, cell, value[a])
                        add(cell, b, ONSITE + b, cell, value[b])
                        add(cell, a, INTRA + layer, cell, value[b])
                        add(cell, b, INTRA + layer, cell, value[a])
                    elif (row_off, col_off) == (-1, 0):
                        add(cell, a, INTRA + 2 + layer, cell, value[b])
                    elif (row_off, col_off) == (1, 0):
                        add(cell, b, INTRA + 2 + layer, step, value[a])
                    elif (row_off, col_off) == (0, -1):
                        add(cell, a, INTRA + 4 + layer, cell, value[b])
                    elif (row_off, col_off) == (0, 1):
                        add(cell, b, INTRA_SHIFTED + layer, cell, value[a])
    return sums


def term_rows(source, target, table, row, value_of):
    lane = lanes_of((V, LANES))
    count = BLOCKS + 1
    keys = [(cell, orbital) for cell in range(2) for orbital in range(4)]
    rows = {key: field_rows(key[1], (row + key[0]) & (RING - 1)) for key in keys}
    up, down = {}, {}

    def columns(block):
        return slice(block * LANES, (block + 1) * LANES)

    def put_up(block):
        for key in keys:
            inner = up[key, block]
            target[0, rows[key], columns(block)] = jnp.where(
                lane == 0, up[key, (block - 1) % count], inner
            )

    def put_down(block):
        for key in keys:
            inner = down[key, block]
            target[2, rows[key], columns(block)] = jnp.where(
                lane == LAST, down[key, (block + 1) % count], inner
            )

    order = [BLOCKS] + list(range(BLOCKS))
    for at, block in enumerate(order):
        result = stencil_pair(source, table, row, block)
        for key in keys:
            value = value_of(result[key[0]][key[1]], rows[key], columns(block))
            target[1, rows[key], columns(block)] = value
            up[key, block] = lane_roll(value, 1)
            down[key, block] = lane_roll(value, -1)
        if at > 0:
            put_up(block)
            put_down(order[at - 1])
    put_up(order[0])
    put_down(order[-1])


def first_term(zero, one, table, row):
    term_rows(zero, one, table, row, lambda sums, rows, cols: 0.5 * sums)


def second_term(zero, one, two, table, row):
    term_rows(one, two, table, row, lambda sums, rows, cols: sums - zero[1, rows, cols])


def inner_kernel(zero_in, table_in, edge, zero, table, one, two):
    edges = registers(edge)
    put_field_rims(zero, edges[:2], range(R))
    put_table_rims(table, edges[2:], 0)

    def first_rows(step, carry):
        first_term(zero, one, table, 2 + 2 * step)
        return carry

    lax.fori_loop(0, 2, first_rows, 0)
    second_term(zero, one, two, table, 3)


def inner(zero, table, edge):
    f32 = jnp.float32
    field = jax.ShapeDtypeStruct(FIELD, f32)
    return pl.pallas_call(
        inner_kernel,
        out_shape=(field, jax.ShapeDtypeStruct((TABLE, LANES), f32), field, field),
        in_specs=[VMEM] * 3,
        out_specs=(VMEM,) * 4,
        input_output_aliases={0: 0, 1: 1},
        compiler_params=pltpu.CompilerParams(vmem_limit_bytes=4 << 20),
        cost_estimate=pl.CostEstimate(flops=8000000, bytes_accessed=8000000, transcendentals=0),
        name="inner",
    )(zero, table, edge)


def terms_kernel(
    zero_in, table_in, one_in, two_in, below_edge, above_edge,
    out, partial, zero, table, one, two, last
):
    lane = lanes_of((V, LANES))
    low = subs_of((R, LANES)) < 4
    below, above = registers(below_edge), registers(above_edge)
    put_field_rims(zero, below[:2], range(R, R + RIM))
    put_field_rims(zero, above[:2], range(RING - RIM, RING))
    put_table_rims(table, [jnp.where(low, b, a) for b, a in zip(below[2:], above[2:])], 1)

    def first_rows(step, carry):
        first_term(zero, one, table, (2 * step - 2 + 4 * (step >> 1)) & (RING - 1))
        return carry

    lax.fori_loop(0, 4, first_rows, 0)

    def second_rows(step, carry):
        second_term(zero, one, two, table, (2 * step - 1 + 2 * (step >> 1)) & (RING - 1))
        return carry

    lax.fori_loop(0, 4, second_rows, 0)

    def third_rows(step, sums):
        row = 2 * step
        sums = list(sums)
        for block in range(BLOCKS):
            cols = slice(block * LANES, (block + 1) * LANES)
            result = stencil_pair(two, table, row, block)
            for cell in range(2):
                for orbital in range(4):
                    rows = field_rows(orbital, row + cell)
                    t0 = zero[1, rows, cols]
                    t1 = one[1, rows, cols]
                    t2 = two[1, rows, cols]
                    t3 = result[cell][orbital] - t1
                    at = pl.multiple_of((orbital * R + row + cell) * V, V)
                    last[pl.ds(at, V), cols] = t3
                    for at, (x, y) in enumerate(
                        ((t0, t0), (t1, t0), (t1, t1), (t2, t1), (t2, t2), (t3, t2), (t3, t3))
                    ):
                        sums[at] = sums[at] + x * y
        return tuple(sums)

    empty = jnp.zeros((V, LANES), jnp.float32)
    sums = lax.fori_loop(0, R // 2, third_rows, (empty,) * 7)

    for orbital in range(4):
        for block in range(BLOCKS):
            cols = slice(block * LANES, (block + 1) * LANES)
            rows = pl.ds(orbital * R * V, R * V)
            turned = jnp.swapaxes(last[rows, cols].reshape(R, V, LANES), 0, 1)
            out[:, orbital, :, cols] = turned

    spread = empty
    sub = subs_of((V, LANES))
    for at in range(7):
        total = jnp.sum(sums[at], axis=1, keepdims=True)
        spread = jnp.where(lane == 8 * at + sub, total, spread)
    line = jnp.sum(spread, axis=0, keepdims=True)
    partial[...] = jnp.broadcast_to(line, partial.shape)


def apply_terms(devices, *args):
    f32 = jnp.float32
    results = pl.pallas_call(
        terms_kernel,
        out_shape=(
            jax.ShapeDtypeStruct((V, 4, R, C), f32),
            jax.ShapeDtypeStruct((devices, LANES), f32),
            jax.ShapeDtypeStruct(FIELD, f32),
            jax.ShapeDtypeStruct((TABLE, LANES), f32),
            jax.ShapeDtypeStruct(FIELD, f32),
            jax.ShapeDtypeStruct(FIELD, f32),
        ),
        in_specs=[VMEM] * 6,
        out_specs=(VMEM,) * 6,
        input_output_aliases={0: 2, 1: 3, 2: 4, 3: 5},
        scratch_shapes=[pltpu.VMEM((4 * R * V, C), f32)],
        compiler_params=pltpu.CompilerParams(vmem_limit_bytes=8 << 20),
        name="terms",
    )(*args)
    return results[0], results[1]


def finish_kernel(orbitals, parts, out):
    line = jnp.sum(parts[...], axis=0, keepdims=True) / orbitals
    rows = [lane_roll(line, -8 * at)[:, 0:V] for at in range(7)]
    out[0:1, :] = rows[0]
    out[1:2, :] = rows[1]
    for at in range(2, 7):
        out[at : at + 1, :] = 2.0 * rows[at] - rows[at % 2]


def finish(parts, orbitals):
    return pl.pallas_call(
        functools.partial(finish_kernel, orbitals),
        out_shape=jax.ShapeDtypeStruct((7, V), jnp.float32),
        in_specs=[VMEM],
        out_specs=VMEM,
        compiler_params=pltpu.CompilerParams(vmem_limit_bytes=1 << 20),
        name="finish",
    )(parts)


def on_device(vectors, onsite, intra_hop, inter_index, inter_hop):
    cols = lax.axis_size("col")
    tiles = lax.axis_size(TILE)
    devices = cols * tiles

    def ring(count, step):
        return [(i, (i + step) % count) for i in range(count)]

    field, coefs, up_msg, down_msg, edge_msg = pack(
        vectors, onsite, intra_hop, inter_index, inter_hop
    )
    right = lax.ppermute(edge_msg, "col", ring(cols, -1))
    left = lax.ppermute(edge_msg, "col", ring(cols, 1))
    below = lax.ppermute(up_msg, TILE, ring(tiles, -1))
    above = lax.ppermute(down_msg, TILE, ring(tiles, 1))
    zero, table = own(field, coefs)
    edge = jnp.where((lanes_of(edge_msg.shape) & 7) < 4, right, left)
    below_edge = lax.ppermute(edge, TILE, ring(tiles, -1))
    above_edge = lax.ppermute(edge, TILE, ring(tiles, 1))
    zero, table, one, two = inner(zero, table, edge)
    zero, table = near(zero, table, below, above)
    last_term, partial = apply_terms(
        devices, zero, table, one, two, below_edge, above_edge
    )
    parts = lax.all_to_all(partial, EVERY, 0, 0)
    return last_term, finish(parts, 4.0 * R * C * devices)


def solution(mesh):
    torus = Mesh(
        mesh.devices.reshape(mesh.shape["col"], 4, 8, 2), ("col", "tile_0", "tile_1", "tile_2")
    )
    placed = (
        P(None, None, TILE, "col"),
        P(None, TILE, "col"),
        P(None, None, TILE, "col"),
        P(None, None, TILE, "col"),
        P(None, None, TILE, "col"),
    )
    return jax.shard_map(
        on_device,
        mesh=torus,
        in_specs=placed,
        out_specs=(P(None, None, TILE, "col"), P()),
        check_vma=False,
    )
```

```python
import functools

import jax
import jax.numpy as jnp
from jax import lax
from jax.experimental import pallas as pl
from jax.experimental.pallas import tpu as pltpu
from jax.sharding import Mesh
from jax.sharding import PartitionSpec as P


TILE = ("tile_0", "tile_1", "tile_2")
EVERY = ("col",) + TILE

V = 8
R = 8
C = 512
W = C + 128
RING = 16
RIM = 3
COEFS = 26
LANES = 128
BLOCKS = C // LANES
LAST = LANES - 1
STEP = RING + 1
VMEM = pl.BlockSpec(memory_space=pltpu.VMEM)
FIELD_ROWS = 4 * RIM * V
TURNED = COEFS // R
PAIR_ROWS = FIELD_ROWS + TURNED * RIM * R
ROW_MSG = PAIR_ROWS + (COEFS - TURNED * R) * 4

FWD = 0
SHIFTED = 36
INTRA = 60
INTRA_SHIFTED = 66
ONSITE = 68
PLANES = 72
STRIDE = PLANES + 1
TABLE = (C // LANES + 1) * RING * STRIDE
FIELD = (3, 4 * STEP * V, W)

SIDE_CODES = [code for code in range(18) if code % 3 != 1]


def offsets(code):
    return code % 9 // 3 - 1, code % 3 - 1


def shifted_plane(source, code):
    if code % 3 == 1:
        return FWD + source * 18 + code
    return SHIFTED + source * 12 + SIDE_CODES.index(code)


def lanes_of(shape):
    return lax.broadcasted_iota(jnp.int32, shape, len(shape) - 1)


def subs_of(shape):
    return lax.broadcasted_iota(jnp.int32, shape, len(shape) - 2)


def lane_roll(array, amount):
    amount = amount % array.shape[-1]
    if amount == 0:
        return array
    return pltpu.roll(array, amount, axis=array.ndim - 1)


def pack_kernel(vec, onsite, intra, codes, inter, field, coefs, up_msg, down_msg, edge_msg):
    for orbital in range(4):
        for block in range(C // LANES):
            cols = slice(block * LANES, (block + 1) * LANES)
            turned = jnp.swapaxes(vec[:, orbital, :, cols], 0, 1)
            for row in range(R):
                field[pl.ds((orbital * R + row) * V, V), cols] = turned[row]
                if row < RIM:
                    up_msg[pl.ds((orbital * RIM + row) * V, V), cols] = turned[row]
                if row >= R - RIM:
                    at = row - (R - RIM)
                    down_msg[pl.ds((orbital * RIM + at) * V, V), cols] = turned[row]

    def plane(index):
        if index < 4:
            return onsite[index]
        if index < 10:
            return intra[(index - 4) // 2, (index - 4) % 2]
        if index < 18:
            return codes[(index - 10) // 2, (index - 10) % 2].astype(jnp.float32)
        return inter[(index - 18) // 2, (index - 18) % 2]

    for index in range(COEFS):
        coefs[pl.ds(index * R, R), :] = plane(index)

    for group in range(TURNED):
        for block in range(BLOCKS):
            cols = slice(block * LANES, (block + 1) * LANES)
            values = coefs[pl.ds(group * R * R, R * R), cols].reshape(R, R, LANES)
            turned = jnp.swapaxes(values, 0, 1)
            for at in range(RIM):
                rows = pl.ds(FIELD_ROWS + (group * RIM + at) * R, R)
                up_msg[rows, cols] = turned[at]
                down_msg[rows, cols] = turned[R - RIM + at]
    low = subs_of((R, C)) < 4
    even, odd = plane(COEFS - 2), pltpu.roll(plane(COEFS - 1), 4, axis=0)
    up_msg[pl.ds(PAIR_ROWS, R), :] = jnp.where(low, even, odd)
    down_msg[pl.ds(PAIR_ROWS, R), :] = jnp.where(low, odd, even)

    lane = lanes_of((R, LANES))

    def pack_edges(count, block_of):
        packed = [jnp.zeros((R, LANES), jnp.float32) for _ in range(2)]
        for slot in range(count):
            ends = jnp.where(lane < 64, block_of(slot, 0), block_of(slot, C - LANES))
            inside = ((lane + 4) & LAST) >> 3 == slot % 16
            packed[slot // 16] = jnp.where(
                inside, lane_roll(ends, 8 * slot), packed[slot // 16]
            )
        return packed

    packed = pack_edges(32, lambda slot, at: field[pl.ds(slot * V, V), at : at + LANES])
    packed += pack_edges(COEFS, lambda slot, at: coefs[pl.ds(slot * R, R), at : at + LANES])
    for at, values in enumerate(packed):
        edge_msg[at * 8 : at * 8 + 8, :] = values


def pack(vectors, onsite, intra, codes, inter):
    f32 = jnp.float32
    return pl.pallas_call(
        pack_kernel,
        out_shape=(
            jax.ShapeDtypeStruct((4 * R * V, C), f32),
            jax.ShapeDtypeStruct((COEFS * R, C), f32),
            jax.ShapeDtypeStruct((ROW_MSG, C), f32),
            jax.ShapeDtypeStruct((ROW_MSG, C), f32),
            jax.ShapeDtypeStruct((32, LANES), f32),
        ),
        out_specs=(VMEM,) * 5,
        compiler_params=pltpu.CompilerParams(vmem_limit_bytes=16 << 20),
        name="pack",
    )(
        *(
            pltpu.with_memory_space_constraint(array, pltpu.HBM)
            for array in (vectors, onsite, intra, codes, inter)
        )
    )


def table_rows(plane, block, half):
    return pl.ds((block * RING + half * R) * STRIDE + plane, R, stride=STRIDE)


def planes_of(plane_at):
    kept = {}
    for index in range(4):
        kept[ONSITE + index] = 2.0 * plane_at(index)
    for index in range(6):
        kept[INTRA + index] = 2.0 * plane_at(4 + index)
    for source in range(2):
        marks = [plane_at(10 + 2 * k + source) for k in range(4)]
        hops = [2.0 * plane_at(18 + 2 * k + source) for k in range(4)]
        for code in range(18):
            terms = [jnp.where(m == float(code), h, 0.0) for m, h in zip(marks, hops)]
            kept[FWD + source * 18 + code] = (terms[0] + terms[1]) + (terms[2] + terms[3])
    return kept


def shifts():
    for source in range(2):
        for code in SIDE_CODES:
            yield FWD + source * 18 + code, shifted_plane(source, code), offsets(code)[1]
    for layer in range(2):
        yield INTRA + 4 + layer, INTRA_SHIFTED + layer, -1


def put_half(table, half, plane_at):
    kept = []
    for block in range(BLOCKS):
        kept.append(planes_of(lambda index: plane_at(index, block)))
        for plane, values in kept[-1].items():
            table[table_rows(plane, block, half), :] = values
    for plane, shifted, amount in shifts():
        row = lane_roll(jnp.concatenate([planes[plane] for planes in kept], axis=1), amount)
        for block in range(BLOCKS):
            at = table_rows(shifted, block, half)
            table[at, :] = row[:, block * LANES : (block + 1) * LANES]


def field_rows(orbital, row):
    return pl.ds((orbital * STEP + row % RING) * V, V)


def put_middle(field, orbital, row, values):
    rows = field_rows(orbital, row)
    field[1, rows, 0:C] = values
    field[0, rows, 0:C] = lane_roll(values, 1)
    field[2, rows, 0:C] = lane_roll(values, -1)


def swap_in(amount, rolled, turned, lane):
    outer = lane == (0 if amount == 1 else LAST)
    return jnp.where(outer, rolled, turned), jnp.where(outer, turned, rolled)


def own_kernel(first, coefs, zero, table):
    for orbital in range(4):
        for row in range(R):
            put_middle(zero, orbital, row, first[pl.ds((orbital * R + row) * V, V), :])

    def plane_at(index, block):
        return coefs[pl.ds(index * R, R), block * LANES : (block + 1) * LANES]

    put_half(table, 0, plane_at)


def own(field, coefs):
    f32 = jnp.float32
    return pl.pallas_call(
        own_kernel,
        out_shape=(
            jax.ShapeDtypeStruct(FIELD, f32),
            jax.ShapeDtypeStruct((TABLE, LANES), f32),
        ),
        in_specs=[VMEM] * 2,
        out_specs=(VMEM,) * 2,
        compiler_params=pltpu.CompilerParams(vmem_limit_bytes=4 << 20),
        cost_estimate=pl.CostEstimate(flops=4000000, bytes_accessed=4000000, transcendentals=0),
        name="own",
    )(field, coefs)


def near_kernel(zero_in, table_in, below, above, zero, table):
    for orbital in range(4):
        for at in range(RIM):
            rows = pl.ds((orbital * RIM + at) * V, V)
            put_middle(zero, orbital, R + at, below[rows, :])
            put_middle(zero, orbital, RING - RIM + at, above[rows, :])
    low = subs_of((R, LANES)) < 4
    turned = {}
    for group in range(TURNED):
        for block in range(BLOCKS):
            cols = slice(block * LANES, (block + 1) * LANES)
            rows = [pl.ds(FIELD_ROWS + (group * RIM + at) * R, R) for at in range(RIM)]
            first = [below[at, cols] for at in rows]
            last = [above[at, cols] for at in rows]
            values = jnp.stack(first + [first[-1], last[0]] + last)
            turned[group, block] = jnp.swapaxes(values, 0, 1)

    def plane_at(index, block):
        if index < TURNED * R:
            return turned[index // R, block][index % R]
        cols = slice(block * LANES, (block + 1) * LANES)
        rows = pl.ds(PAIR_ROWS, R)
        if index % 2 == 0:
            return jnp.where(low, below[rows, cols], above[rows, cols])
        return pltpu.roll(jnp.where(low, above[rows, cols], below[rows, cols]), 4, axis=0)

    put_half(table, 1, plane_at)


def near(zero, table, below, above):
    f32 = jnp.float32
    return pl.pallas_call(
        near_kernel,
        out_shape=(
            jax.ShapeDtypeStruct(FIELD, f32),
            jax.ShapeDtypeStruct((TABLE, LANES), f32),
        ),
        in_specs=[VMEM] * 4,
        out_specs=(VMEM,) * 2,
        input_output_aliases={0: 0, 1: 1},
        compiler_params=pltpu.CompilerParams(vmem_limit_bytes=4 << 20),
        cost_estimate=pl.CostEstimate(flops=4000000, bytes_accessed=4000000, transcendentals=0),
        name="near",
    )(zero, table, below, above)


def put_field_rims(zero, edges, ring_rows):
    lane = lanes_of((V, LANES))
    for orbital in range(4):
        stores = []
        for row in ring_rows:
            slot = orbital * 8 + row % 8
            rims = [lane_roll(edges[slot // 16], amount - 8 * slot) for amount in (1, 0, -1)]
            rows = field_rows(orbital, row)
            first = swap_in(1, rims[0], zero[0, rows, 0:LANES], lane)
            last = swap_in(-1, rims[2], zero[2, rows, C - LANES : C], lane)
            stores.append((rows, rims[1], first, last))
        for rows, rim, first, last in stores:
            zero[1, rows, C:W] = rim
            zero[0, rows, 0:LANES], zero[0, rows, C:W] = first
            zero[2, rows, C - LANES : C], zero[2, rows, C:W] = last


def put_table_rims(table, edges, half):
    lane = lanes_of((R, LANES))

    def rolled_by(amount):
        return lambda index: lane_roll(edges[index // 16], amount - 8 * index)

    for plane, values in planes_of(rolled_by(0)).items():
        table[table_rows(plane, BLOCKS, half), :] = values
    for amount in (1, -1):
        rolled = planes_of(rolled_by(amount))
        for plane, shifted, by in shifts():
            if by == amount:
                at = table_rows(shifted, 0 if amount == 1 else BLOCKS - 1, half)
                edge, outer = swap_in(amount, rolled[plane], table[at, :], lane)
                table[at, :] = edge
                table[table_rows(shifted, BLOCKS, half), :] = outer


def registers(edge):
    return [edge[8 * at : 8 * at + 8, :] for at in range(4)]


def stencil_pair(field, table, pair, block):
    cols = slice(block * LANES, (block + 1) * LANES)

    def start(row):
        return (block * RING + row % RING) * STRIDE

    sums = [[None] * 4 for _ in range(2)]

    def add(cell, orbital, plane, row, value):
        coef = table[pl.ds(start(row) + plane, V, stride=0), :]
        term = coef * value
        old = sums[cell][orbital]
        sums[cell][orbital] = term if old is None else old + term

    for there in sorted({row + step for row in pair for step in (-1, 0, 1)}):
        for col_off in (-1, 0, 1):
            value = [field[1 + col_off, field_rows(o, there), cols] for o in range(4)]
            for cell, here in enumerate(pair):
                row_off = there - here
                if abs(row_off) > 1:
                    continue
                code = (row_off + 1) * 3 + col_off + 1
                back = (1 - row_off) * 3 + 1 - col_off
                for source in range(2):
                    for target in range(2):
                        plane = FWD + source * 18 + 9 * target + code
                        add(cell, source, plane, here, value[2 + target])
                        plane = shifted_plane(source, 9 * target + back)
                        add(cell, 2 + target, plane, there, value[source])
                for layer in range(2):
                    a, b = 2 * layer, 2 * layer + 1
                    if (row_off, col_off) == (0, 0):
                        add(cell, a, ONSITE + a, here, value[a])
                        add(cell, b, ONSITE + b, here, value[b])
                        add(cell, a, INTRA + layer, here, value[b])
                        add(cell, b, INTRA + layer, here, value[a])
                    elif (row_off, col_off) == (-1, 0):
                        add(cell, a, INTRA + 2 + layer, here, value[b])
                    elif (row_off, col_off) == (1, 0):
                        add(cell, b, INTRA + 2 + layer, there, value[a])
                    elif (row_off, col_off) == (0, -1):
                        add(cell, a, INTRA + 4 + layer, here, value[b])
                    elif (row_off, col_off) == (0, 1):
                        add(cell, b, INTRA_SHIFTED + layer, here, value[a])
    return sums


def term_rows(source, target, table, pair, value_of):
    lane = lanes_of((V, LANES))
    count = BLOCKS + 1
    keys = [(cell, orbital) for cell in range(2) for orbital in range(4)]
    rows = {key: field_rows(key[1], pair[key[0]]) for key in keys}
    up, down = {}, {}

    def columns(block):
        return slice(block * LANES, (block + 1) * LANES)

    def put_up(block):
        for key in keys:
            inner = up[key, block]
            target[0, rows[key], columns(block)] = jnp.where(
                lane == 0, up[key, (block - 1) % count], inner
            )

    def put_down(block):
        for key in keys:
            inner = down[key, block]
            target[2, rows[key], columns(block)] = jnp.where(
                lane == LAST, down[key, (block + 1) % count], inner
            )

    order = [BLOCKS] + list(range(BLOCKS))
    for at, block in enumerate(order):
        result = stencil_pair(source, table, pair, block)
        for key in keys:
            value = value_of(result[key[0]][key[1]], rows[key], columns(block))
            target[1, rows[key], columns(block)] = value
            up[key, block] = lane_roll(value, 1)
            down[key, block] = lane_roll(value, -1)
        if at > 0:
            put_up(block)
            put_down(order[at - 1])
    put_up(order[0])
    put_down(order[-1])


def first_term(zero, one, table, pair):
    term_rows(zero, one, table, pair, lambda sums, rows, cols: 0.5 * sums)


def second_term(zero, one, two, table, pair):
    term_rows(one, two, table, pair, lambda sums, rows, cols: sums - zero[1, rows, cols])


def inner_kernel(zero_in, table_in, edge, zero, table, one, two):
    edges = registers(edge)
    put_field_rims(zero, edges[:2], range(R))
    put_table_rims(table, edges[2:], 0)

    for pair in ((1, 2), (3, 4), (5, 6)):
        first_term(zero, one, table, pair)
    for pair in ((2, 3), (4, 5)):
        second_term(zero, one, two, table, pair)


def inner(zero, table, edge):
    f32 = jnp.float32
    field = jax.ShapeDtypeStruct(FIELD, f32)
    return pl.pallas_call(
        inner_kernel,
        out_shape=(field, jax.ShapeDtypeStruct((TABLE, LANES), f32), field, field),
        in_specs=[VMEM] * 3,
        out_specs=(VMEM,) * 4,
        input_output_aliases={0: 0, 1: 1},
        compiler_params=pltpu.CompilerParams(vmem_limit_bytes=4 << 20),
        cost_estimate=pl.CostEstimate(flops=8000000, bytes_accessed=8000000, transcendentals=0),
        name="inner",
    )(zero, table, edge)


def terms_kernel(
    zero_in, table_in, one_in, two_in, below_edge, above_edge,
    out, partial, zero, table, one, two, last, turned, sems
):
    lane = lanes_of((V, LANES))
    low = subs_of((R, LANES)) < 4
    below, above = registers(below_edge), registers(above_edge)
    put_field_rims(zero, below[:2], range(R, R + RIM))
    put_field_rims(zero, above[:2], range(RING - RIM, RING))
    put_table_rims(table, [jnp.where(low, b, a) for b, a in zip(below[2:], above[2:])], 1)

    for pair in ((-2, -1), (0, 7), (8, 9)):
        first_term(zero, one, table, pair)
    for pair in ((-1, 0), (1, 6), (7, 8)):
        second_term(zero, one, two, table, pair)

    empty = jnp.zeros((V, LANES), jnp.float32)
    sums = [empty] * 7
    copies = []
    for block in range(BLOCKS):
        cols = slice(block * LANES, (block + 1) * LANES)
        for pair in ((0, 1), (2, 3), (4, 5), (6, 7)):
            result = stencil_pair(two, table, pair, block)
            for cell, row in enumerate(pair):
                for orbital in range(4):
                    rows = field_rows(orbital, row)
                    t0 = zero[1, rows, cols]
                    t1 = one[1, rows, cols]
                    t2 = two[1, rows, cols]
                    t3 = result[cell][orbital] - t1
                    last[pl.ds((orbital * R + row) * V, V), cols] = t3
                    for at, (x, y) in enumerate(
                        ((t0, t0), (t1, t0), (t1, t1), (t2, t1), (t2, t2), (t3, t2), (t3, t3))
                    ):
                        sums[at] = sums[at] + x * y
        for orbital in range(4):
            rows = pl.ds(orbital * R * V, R * V)
            values = last[rows, cols].reshape(R, V, LANES)
            turned[:, orbital, :, cols] = jnp.swapaxes(values, 0, 1)
        copies.append(
            pltpu.make_async_copy(
                turned.at[:, :, :, cols], out.at[:, :, :, cols], sems.at[block]
            )
        )
        if block > 0:
            copies[block - 1].start()

    spread = empty
    sub = subs_of((V, LANES))
    for at in range(7):
        total = jnp.sum(sums[at], axis=1, keepdims=True)
        spread = jnp.where(lane == 8 * at + sub, total, spread)
    line = jnp.sum(spread, axis=0, keepdims=True)
    partial[...] = jnp.broadcast_to(line, partial.shape)
    copies[-1].start()
    for copy in copies:
        copy.wait()


def apply_terms(devices, *args):
    f32 = jnp.float32
    results = pl.pallas_call(
        terms_kernel,
        out_shape=(
            jax.ShapeDtypeStruct((V, 4, R, C), f32),
            jax.ShapeDtypeStruct((devices, LANES), f32),
            jax.ShapeDtypeStruct(FIELD, f32),
            jax.ShapeDtypeStruct((TABLE, LANES), f32),
            jax.ShapeDtypeStruct(FIELD, f32),
            jax.ShapeDtypeStruct(FIELD, f32),
        ),
        in_specs=[VMEM] * 6,
        out_specs=(pl.BlockSpec(memory_space=pltpu.HBM),) + (VMEM,) * 5,
        input_output_aliases={0: 2, 1: 3, 2: 4, 3: 5},
        scratch_shapes=[
            pltpu.VMEM((4 * R * V, C), f32),
            pltpu.VMEM((V, 4, R, C), f32),
            pltpu.SemaphoreType.DMA((BLOCKS,)),
        ],
        compiler_params=pltpu.CompilerParams(vmem_limit_bytes=8 << 20),
        name="terms",
    )(*args)
    return results[0], results[1]


def finish_kernel(orbitals, parts, out):
    line = jnp.sum(parts[...], axis=0, keepdims=True) / orbitals
    rows = [lane_roll(line, -8 * at)[:, 0:V] for at in range(7)]
    out[0:1, :] = rows[0]
    out[1:2, :] = rows[1]
    for at in range(2, 7):
        out[at : at + 1, :] = 2.0 * rows[at] - rows[at % 2]


def finish(parts, orbitals):
    return pl.pallas_call(
        functools.partial(finish_kernel, orbitals),
        out_shape=jax.ShapeDtypeStruct((7, V), jnp.float32),
        in_specs=[VMEM],
        out_specs=VMEM,
        compiler_params=pltpu.CompilerParams(vmem_limit_bytes=1 << 20),
        name="finish",
    )(parts)


def on_device(vectors, onsite, intra_hop, inter_index, inter_hop):
    cols = lax.axis_size("col")
    tiles = lax.axis_size(TILE)
    devices = cols * tiles

    def ring(count, step):
        return [(i, (i + step) % count) for i in range(count)]

    field, coefs, up_msg, down_msg, edge_msg = pack(
        vectors, onsite, intra_hop, inter_index, inter_hop
    )
    right = lax.ppermute(edge_msg, "col", ring(cols, -1))
    left = lax.ppermute(edge_msg, "col", ring(cols, 1))
    below = lax.ppermute(up_msg, TILE, ring(tiles, -1))
    above = lax.ppermute(down_msg, TILE, ring(tiles, 1))
    zero, table = own(field, coefs)
    edge = jnp.where((lanes_of(edge_msg.shape) & 7) < 4, right, left)
    below_edge = lax.ppermute(edge, TILE, ring(tiles, -1))
    above_edge = lax.ppermute(edge, TILE, ring(tiles, 1))
    zero, table, one, two = inner(zero, table, edge)
    zero, table = near(zero, table, below, above)
    last_term, partial = apply_terms(
        devices, zero, table, one, two, below_edge, above_edge
    )
    parts = lax.all_to_all(partial, EVERY, 0, 0)
    return last_term, finish(parts, 4.0 * R * C * devices)


def solution(mesh):
    torus = Mesh(
        mesh.devices.reshape(mesh.shape["col"], 4, 8, 2), ("col", "tile_0", "tile_1", "tile_2")
    )
    placed = (
        P(None, None, TILE, "col"),
        P(None, TILE, "col"),
        P(None, None, TILE, "col"),
        P(None, None, TILE, "col"),
        P(None, None, TILE, "col"),
    )
    return jax.shard_map(
        on_device,
        mesh=torus,
        in_specs=placed,
        out_specs=(P(None, None, TILE, "col"), P()),
        check_vma=False,
    )
```
